32 devices in a mesh: groups: 2 (over x), blk: 8 (over z, y), rep: 2 (over core).
Axes of the slice: x: 2, y: 2, z: 4, core: 2. Of those that a mesh axis runs over, the one named last changes fastest.
Arguments:
- resident: bfloat16 [32768, 768], P(('groups', 'blk', 'rep')), parts along dimension 0, may hold values from -600 to 600
- ingest: bfloat16 [16384, 768], P(('groups', 'blk', 'rep')), parts along dimension 0, may hold values from -600 to 600
- cluster_ids: int32 [16384], P(('groups', 'blk', 'rep')), parts along dimension 0, may hold values from 0 to 127, as said below
Outputs:
- resident_score: float32 [32768], P(('groups', 'blk', 'rep')), parts along dimension 0
- ingest_score: float32 [16384], P(('groups', 'blk', 'rep')), parts along dimension 0
The draws below stay inside these ranges and needn't reach their ends.
There are 2 independent parts, one for each index of `groups`. The reference program is written for one: setup_inputs(seed, part) draws one part's arguments, and reference() takes and returns one part's arrays. A program takes and returns all parts, laid end to end along the dimension named above; each array names one. Nothing has to cross between parts.
Inputs may be any that keep to these rules, and one draw needn't show every extreme that they name: `cluster_ids`: clusters 16 * p to 16 * p + 15 belong to cycle position p. At most 96 documents of one device belong to one cycle position, and in every draw some cycle position receives 96 from every device.
All inputs are finite; a program needn't handle non-finite values.
Results may differ from the reference program's by a relative error of at most 0.0003.
Values may be sent and summed in bfloat16 or wider, within the bound.
A program may use at most 64 MiB of HBM per device.

```python
import jax
import jax.numpy as jnp
from jax import lax

D = 768
INGEST_DEV = 512
CL_OWN = 16
CYCLE_STEPS = 4
CAP = 96
VISIT = 1536
RES_POS = 2048
RESIDENT = 16384
INGEST = 8192
CLUSTERS = 128
N_BLK = 8
N_REP = 2


def slot_layout(key):
    base = jax.random.fold_in(key, 7)
    sources = N_BLK * N_REP
    slot_total = N_BLK * CAP
    weights = jax.random.randint(jax.random.fold_in(base, 1), (N_BLK,), 1, 9)
    heavy = jax.random.randint(jax.random.fold_in(base, 2), (), 0, N_BLK)
    raw = jax.random.randint(jax.random.fold_in(base, 3), (sources, N_BLK, CAP), 0, 1024) * weights[None, :, None]
    owner_grid = jnp.arange(N_BLK, dtype=jnp.int32)[None, :, None]
    raw = raw + jnp.where(owner_grid == heavy, 16384, 0)
    ordering = jnp.arange(slot_total, dtype=jnp.int32).reshape(1, N_BLK, CAP)
    scores = (raw * slot_total + ordering).reshape(sources, slot_total)
    chosen = lax.top_k(scores, INGEST_DEV)[1]
    shuffle_bits = jax.random.randint(jax.random.fold_in(base, 4), (sources, INGEST_DEV), 0, 2 ** 20)
    shuffle_keys = shuffle_bits * INGEST_DEV + jnp.arange(INGEST_DEV, dtype=jnp.int32)[None, :]
    shuffled = jnp.take_along_axis(chosen, jnp.argsort(shuffle_keys, axis=1), axis=1)
    owners = shuffled // CAP
    within = jax.random.randint(jax.random.fold_in(base, 5), (sources, INGEST_DEV), 0, CL_OWN)
    return (owners * CL_OWN + within).reshape(-1).astype(jnp.int32)


def centroid_table(key):
    base = jax.random.fold_in(key, 101)
    span = 6 * CL_OWN
    basis = jax.random.truncated_normal(jax.random.fold_in(base, 1), -5.0, 5.0, (CLUSTERS, D), jnp.float32)
    indices = jnp.arange(CLUSTERS, dtype=jnp.int32)
    band = ((indices[None, :] - indices[:, None]) % CLUSTERS < span).astype(jnp.float32)
    centres = jnp.dot(band, basis, precision=lax.Precision.HIGHEST) / jnp.sqrt(jnp.float32(min(span, CLUSTERS)))
    spread = jnp.exp(jax.random.uniform(jax.random.fold_in(base, 2), (CLUSTERS,), jnp.float32, jnp.log(0.4), jnp.log(2.0)))
    return (centres, spread)


def embed_rows(key, clusters, salt):
    centres, spread = centroid_table(key)
    salted = jax.random.fold_in(key, salt)
    count = clusters.shape[0]
    jitter = jax.random.truncated_normal(jax.random.fold_in(salted, 1), -5.0, 5.0, (count, D), jnp.float32)
    scales = jnp.exp(jax.random.uniform(jax.random.fold_in(salted, 2), (count,), jnp.float32, 0.0, jnp.log(10.0)))
    rows = (0.5 * centres[clusters] + spread[clusters][:, None] * jitter) * scales[:, None]
    return rows.astype(jnp.bfloat16)


def draw_resident(key, part):
    positions = jnp.arange(RESIDENT, dtype=jnp.int32) // RES_POS
    within = jax.random.randint(jax.random.fold_in(key, 201), (RESIDENT,), 0, CL_OWN)
    return embed_rows(key, positions * CL_OWN + within, 202)


def draw_ingest(key, part):
    clusters = slot_layout(key)
    rows = embed_rows(key, clusters, 203).astype(jnp.float32)
    resident_rows = draw_resident(key, part).astype(jnp.float32)
    base = jax.random.fold_in(key, 301)
    owners = clusters // CL_OWN
    offsets = jax.random.randint(jax.random.fold_in(base, 1), (INGEST,), 1, CYCLE_STEPS + 1)
    picks = jax.random.randint(jax.random.fold_in(base, 2), (INGEST,), 0, RES_POS)
    sources = (owners + offsets) % N_BLK * RES_POS + picks
    copied = resident_rows[sources]
    level = jnp.sqrt(jnp.mean(copied * copied, axis=1) + 1e-12)
    noise = jax.random.truncated_normal(jax.random.fold_in(base, 3), -3.0, 3.0, (INGEST, D), jnp.float32)
    factor = jax.random.uniform(jax.random.fold_in(base, 4), (INGEST,), jnp.float32, 0.5, 1.0)
    near = (copied + 0.02 * level[:, None] * noise) * factor[:, None]
    planted = jax.random.randint(jax.random.fold_in(base, 5), (INGEST,), 0, 4) == 0
    rows = jnp.where(planted[:, None], near, rows)
    return rows.astype(jnp.bfloat16)


def draw_cluster_ids(key, part):
    return slot_layout(key)


def setup_inputs(seed: int = 0, part: int = 0) -> dict:
    splits = jax.random.split(jax.random.key(seed), 4)
    part_keys = jax.random.split(jax.random.fold_in(splits[3], part), 4)
    resident = draw_resident(jax.random.fold_in(jax.random.fold_in(splits[3], part), 71), part)
    ingest = draw_ingest(jax.random.fold_in(jax.random.fold_in(splits[3], part), 71), part)
    cluster_ids = draw_cluster_ids(jax.random.fold_in(jax.random.fold_in(splits[3], part), 71), part)
    return {"resident": resident, "ingest": ingest, "cluster_ids": cluster_ids}


temper = 0.2
epsilon = 1e-06

def unit_rows(rows):
    values = rows.astype(jnp.float32)
    squares = lax.optimization_barrier(jnp.sum(values * values, axis=-1, keepdims=True)) + epsilon
    factor = lax.rsqrt(squares)
    return (values * factor).astype(jnp.bfloat16)

def reference(resident, ingest, cluster_ids):
    unit_resident = unit_rows(resident).reshape(N_BLK, RES_POS, D)
    unit_ingest = unit_rows(ingest)
    owners = cluster_ids // CL_OWN
    sources = N_BLK * N_REP
    grouped = owners.reshape(sources, INGEST_DEV)
    onehot = (grouped[:, :, None] == jnp.arange(N_BLK, dtype=jnp.int32)[None, None, :]).astype(jnp.int32)
    rank_within = lax.optimization_barrier(jnp.sum((jnp.cumsum(onehot, axis=1) - onehot) * onehot, axis=2))
    source_ids = jnp.arange(sources, dtype=jnp.int32)[:, None]
    slot_index = (source_ids % N_REP * (N_BLK * CAP) + source_ids // N_REP * CAP + rank_within).reshape(INGEST)
    visiting = jnp.zeros((N_BLK, VISIT, D), jnp.bfloat16).at[owners, slot_index].set(unit_ingest)
    occupied = jnp.zeros((N_BLK, VISIT), jnp.float32).at[owners, slot_index].set(1.0)

    def per_owner(pieces):
        position, visitors, occupancy = pieces
        visit_sum = jnp.zeros((VISIT,), jnp.float32)
        partials = []
        for offset in range(CYCLE_STEPS + 1):
            resident_block = lax.dynamic_index_in_dim(unit_resident, (position + offset) % N_BLK, 0, keepdims=False)
            scores = jnp.dot(visitors, resident_block.T, preferred_element_type=jnp.float32)
            kernel = jnp.exp((scores - 1.0) / temper)
            visit_sum = visit_sum + lax.optimization_barrier(jnp.sum(kernel, axis=1))
            partials.append(lax.optimization_barrier(jnp.sum(kernel * occupancy[:, None], axis=0)))
        return (visit_sum, jnp.stack(partials))
    visit_sums, resident_parts = lax.map(per_owner, (jnp.arange(N_BLK, dtype=jnp.int32), visiting, occupied))
    resident_density = resident_parts[:, 0]
    for offset in range(1, CYCLE_STEPS + 1):
        resident_density = resident_density + jnp.roll(resident_parts[:, offset], offset, axis=0)
    ingest_density = visit_sums[owners, slot_index]
    return (jnp.log1p(resident_density.reshape(RESIDENT)), jnp.log1p(ingest_density))
```

```python
import functools
import math

import jax
import jax.numpy as jnp
from jax import lax
from jax.experimental import pallas as pl
from jax.experimental.pallas import tpu as pltpu
from jax.sharding import PartitionSpec as P

INGEST_DEV = 512
CL_OWN = 16
CYCLE_STEPS = 4


temper = 0.2
epsilon = 1e-06


def shifted(value, axis, steps):
    count = lax.axis_size(axis)
    pairs = [(source, (source + steps) % count) for source in range(count)]
    return lax.ppermute(value, axis, pairs)


def unit_rows(rows):
    values = rows.astype(jnp.float32)
    squares = jnp.sum(values * values, axis=-1, keepdims=True) + epsilon
    factor = lax.rsqrt(squares)
    return (values * factor).astype(jnp.bfloat16)


def kernel_sums(visitors, occupancy, residents):
    count_rows = visitors.shape[0]
    block_rows = 512
    num_blocks = count_rows // block_rows
    visit_blocks = visitors.reshape(num_blocks, block_rows, visitors.shape[1])
    live_blocks = occupancy.astype(jnp.float32).reshape(num_blocks, block_rows)

    def tile_sums(running, pieces):
        visit_tile, live_tile = pieces
        scores = jnp.einsum("vd,rd->vr", visit_tile, residents, preferred_element_type=jnp.float32)
        kernel = jnp.exp((scores - 1.0) / temper)
        return (running + jnp.sum(kernel * live_tile[:, None], axis=0), jnp.sum(kernel, axis=1))

    resident_part, visit_parts = lax.scan(
        tile_sums, jnp.zeros((residents.shape[0],), jnp.float32), (visit_blocks, live_blocks)
    )
    return (visit_parts.reshape(count_rows), resident_part)


def on_device(resident, ingest, cluster_ids):
    cycle_size = lax.axis_size("blk")
    slot_count = 3 * INGEST_DEV // (2 * cycle_size)
    columns = ingest.shape[1]
    owners = cluster_ids // CL_OWN
    onehot = (owners[:, None] == jnp.arange(cycle_size, dtype=jnp.int32)[None, :]).astype(jnp.int32)
    rank_within = jnp.sum((jnp.cumsum(onehot, axis=0) - onehot) * onehot, axis=1)
    targets = owners * slot_count + rank_within
    unit_ingest = unit_rows(ingest)
    outgoing = (
        jnp.zeros((cycle_size * slot_count, columns), jnp.bfloat16).at[targets].set(unit_ingest)
    )
    filled = (
        jnp.zeros((cycle_size * slot_count,), jnp.bfloat16)
        .at[targets]
        .set(jnp.ones((ingest.shape[0],), jnp.bfloat16))
    )
    arrived, present = (
        lax.all_to_all(
            outgoing.reshape(cycle_size, slot_count, columns),
            "blk",
            split_axis=0,
            concat_axis=0,
            tiled=True,
        ),
        lax.all_to_all(
            filled.reshape(cycle_size, slot_count), "blk", split_axis=0, concat_axis=0, tiled=True
        ),
    )
    visitors, marked = (
        lax.all_gather(
            arrived.reshape(cycle_size * slot_count, columns), "rep", axis=0, tiled=True
        ),
        lax.all_gather(present.reshape(cycle_size * slot_count), "rep", axis=0, tiled=True),
    )
    unit_resident = unit_rows(resident)
    visit_total = jnp.zeros((visitors.shape[0],), jnp.float32)
    resident_total = jnp.zeros((resident.shape[0],), jnp.float32)
    moving = unit_resident
    for rotation in range(CYCLE_STEPS + 1):
        if rotation > 0:
            moving = shifted(moving, "blk", -1)
            resident_total = shifted(resident_total, "blk", -1)
        visit_part, resident_part = kernel_sums(visitors, marked, moving)
        visit_total = visit_total + visit_part
        resident_total = resident_total + resident_part
    resident_total = shifted(resident_total, "blk", CYCLE_STEPS)
    own_sums = lax.psum_scatter(visit_total, "rep", scatter_dimension=0, tiled=True)
    returned = lax.all_to_all(
        own_sums.reshape(cycle_size, slot_count), "blk", split_axis=0, concat_axis=0, tiled=True
    )
    density = returned.reshape(cycle_size * slot_count)[targets]
    return (jnp.log1p(resident_total), jnp.log1p(density))


PAIR = 2
LANES = 128
SUBLANES = 8
INGEST_CHUNK = 256
RESIDENT_CHUNK = 256
HALVES = 2
MESH = pl.DeviceIdType.MESH


def dense_kernel(
    cycle, ids_ref, ingest_ref, resident_ref, resident_out, ingest_out,
    raw_ingest, raw_resident, load_sem, rows, bank, ids, by_resident, by_ingest, resident_sums, ingest_sums, resident_terms, ingest_terms,
    up_send, down_send, rows_recv, up_ids_send, down_ids_send, ids_recv, peer_send, peer_recv, core_send, core_recv,
    relay_send, relay_recv, part_send, part_recv, term_send, term_recv,
):
    line_size = cycle // PAIR
    me = lax.axis_index("blk")
    core = lax.axis_index("rep")
    line, side = me // PAIR, me % PAIR
    chunks = ingest_ref.shape[0] // INGEST_CHUNK
    held = resident_ref.shape[0]
    pieces = held // RESIDENT_CHUNK
    tile_rows = 2 * held
    steps = (line_size - 1) * chunks
    half_rows = INGEST_CHUNK // HALVES
    at_end = (line == 0) | (line == line_size - 1)
    below_end, above_end = line == 1, line == line_size - 2
    holds_back = line_size > 2

    def device(at_line, at_side, at_core):
        return {"blk": at_line * PAIR + at_side, "rep": at_core}

    sibling = device(line, side, 1 - core)
    peer = device(line, 1 - side, core)
    across = device(line, 1 - side, 1 - core)

    def remote(source, target, send, recv, where):
        return pltpu.make_async_remote_copy(
            src_ref=source, dst_ref=target, send_sem=send, recv_sem=recv, device_id=where, device_id_type=MESH
        )

    def row_copy(c, h, send, where):
        part = rows.at[c, pl.ds(h * half_rows, half_rows)]
        return remote(part, part, send.at[c, h], rows_recv.at[c, h], where)

    def id_copy(c, send, where):
        return remote(ids.at[c], ids.at[c], send.at[c], ids_recv.at[c], where)

    above, below = device(line + 1, side, core), device(line - 1, side, core)

    def up_copies(c):
        return [id_copy(c, up_ids_send, above)] + [row_copy(c, h, up_send, above) for h in range(HALVES)]

    def down_copies(c):
        return [id_copy(c, down_ids_send, below)] + [row_copy(c, h, down_send, below) for h in range(HALVES)]

    def start_all(copies):
        for copy in copies:
            copy.start()

    def peer_copy(m):
        return remote(
            bank.at[pl.ds(m * RESIDENT_CHUNK, RESIDENT_CHUNK)],
            bank.at[pl.ds(2 * held + m * RESIDENT_CHUNK, RESIDENT_CHUNK)],
            peer_send.at[m], peer_recv.at[m], peer,
        )

    def relay_copy(m):
        return remote(
            bank.at[pl.ds(2 * held + m * RESIDENT_CHUNK, RESIDENT_CHUNK)],
            bank.at[pl.ds(3 * held + m * RESIDENT_CHUNK, RESIDENT_CHUNK)],
            relay_send.at[m], relay_recv.at[m], sibling,
        )

    core_copy = remote(bank.at[pl.ds(0, held)], bank.at[pl.ds(held, held)], core_send, core_recv, sibling)

    def term_copy(other):
        return remote(
            ingest_sums.at[pl.ds(other * chunks, chunks)], ingest_terms.at[pl.ds(line * chunks, chunks)],
            term_send.at[other], term_recv.at[line], device(other, side, core),
        )

    def term_arrival(other):
        return remote(
            ingest_sums.at[pl.ds(other * chunks, chunks)], ingest_terms.at[pl.ds(other * chunks, chunks)],
            term_send.at[other], term_recv.at[other], device(other, side, core),
        )

    def part_copy(slot):
        return remote(
            resident_sums.at[slot], resident_terms.at[slot], part_send.at[slot], part_recv.at[slot],
            (None, sibling, peer, across)[slot],
        )

    barrier = pltpu.get_barrier_semaphore()
    for where in (sibling, peer, across):
        pl.semaphore_signal(barrier, inc=1, device_id=where, device_id_type=MESH)

    @pl.when(line > 0)
    def _():
        pl.semaphore_signal(barrier, inc=1, device_id=below, device_id_type=MESH)

    @pl.when(line + 1 < line_size)
    def _():
        pl.semaphore_signal(barrier, inc=1, device_id=above, device_id_type=MESH)

    ingest_load = pltpu.make_async_copy(ingest_ref, raw_ingest, load_sem.at[0])
    resident_load = pltpu.make_async_copy(resident_ref, raw_resident, load_sem.at[1])
    ids_load = pltpu.make_async_copy(ids_ref, ids.at[pl.ds(line * chunks, chunks)], load_sem.at[2])
    for load in (ingest_load, ids_load, resident_load):
        load.start()

    def unit(block):
        values = block.astype(jnp.float32)
        squares = jnp.sum(values * values, axis=-1, keepdims=True) + epsilon
        return (values * lax.rsqrt(squares)).astype(jnp.bfloat16)

    ingest_load.wait()
    for j in range(chunks):
        rows[line * chunks + j] = unit(raw_ingest[j * INGEST_CHUNK:(j + 1) * INGEST_CHUNK, :])
    ids_load.wait()
    pl.semaphore_wait(barrier, 3 + (line > 0).astype(jnp.int32) + (line + 1 < line_size).astype(jnp.int32))
    for j in range(chunks):
        kept = holds_back and j == chunks - 1

        @pl.when((line + 1 < line_size) & jnp.logical_not(above_end & kept))
        def _():
            start_all(up_copies(line * chunks + j))

        @pl.when((line > 0) & jnp.logical_not(below_end & kept))
        def _():
            start_all(down_copies(line * chunks + j))

    resident_load.wait()

    @pl.loop(0, pieces)
    def _(m):
        part = pl.ds(m * RESIDENT_CHUNK, RESIDENT_CHUNK)
        bank[part, :] = unit(raw_resident[part, :])

    for m in range(pieces):
        peer_copy(m).start()
    core_copy.start()
    by_resident[...] = jnp.zeros_like(by_resident)
    by_ingest[...] = jnp.zeros_like(by_ingest)

    scale = math.log2(math.e) / temper
    span = CL_OWN * cycle

    def work(c, first, last):
        @pl.loop(first, last)
        def _(tile):
            part = pl.ds(pl.multiple_of(tile * tile_rows, tile_rows), tile_rows)
            position = line * PAIR + jnp.where(tile == 0, side, 1 - side)
            gap = (position + 1) * CL_OWN - 1 - ids[c]
            gap = jnp.where(gap < 0, gap + span, gap)
            bias = jnp.where(gap < CL_OWN * (CYCLE_STEPS + 1), -scale, -1e30)
            scores = lax.dot_general(
                bank[part, :], rows[c], (((1,), (1,)), ((), ())), preferred_element_type=jnp.float32
            )
            kernel = jnp.exp2(scores * scale + bias)
            by_ingest[c] += jnp.sum(kernel.reshape(tile_rows // SUBLANES, SUBLANES, INGEST_CHUNK), axis=0)
            folded = kernel[:, :LANES]
            for n in range(1, INGEST_CHUNK // LANES):
                folded = folded + kernel[:, n * LANES:(n + 1) * LANES]
            by_resident[part, :] += folded

    core_copy.wait_recv()

    @pl.loop(0, chunks)
    def _(j):
        work(line * chunks + j, 0, 1)

    def place(step):
        if not holds_back:
            return step
        turned = jnp.where(step == 0, 0, step + chunks - 1)
        late = step >= steps - chunks + 1
        return jnp.where(at_end & (chunks > 1), jnp.where(late, step - (steps - chunks), turned), step)

    def rank(spot):
        if not holds_back:
            return spot
        turned = jnp.where(spot == 0, 0, spot - chunks + 1)
        late = (spot >= 1) & (spot < chunks)
        return jnp.where(at_end & (chunks > 1), jnp.where(late, spot + steps - chunks, turned), spot)

    def take(step):
        spot = place(step)
        hop, j = spot // chunks + 1, spot % chunks

        @pl.when(line - hop >= 0)
        def _():
            for copy in up_copies((line - hop) * chunks + j):
                copy.wait_recv()

                @pl.when(line + 1 < line_size)
                def _():
                    copy.start()

        @pl.when(line + hop < line_size)
        def _():
            for copy in down_copies((line + hop) * chunks + j):
                copy.wait_recv()

                @pl.when(line > 0)
                def _():
                    copy.start()

        if holds_back:
            @pl.when((step == (line_size - 2) * chunks - 1) & above_end)
            def _():
                start_all(up_copies(line * chunks + chunks - 1))

            @pl.when((step == (line_size - 2) * chunks - 1) & below_end)
            def _():
                start_all(down_copies(line * chunks + chunks - 1))

        @pl.when(step < pieces)
        def _():
            peer_copy(step).wait_recv()
            relay_copy(step).start()

        @pl.loop(0, 2)
        def _(way):
            other = line + (2 * way - 1) * hop

            @pl.when((other >= 0) & (other < line_size))
            def _():
                work(other * chunks + j, 0, jnp.where(step < pieces, 1, 2))

        @pl.when(step == pieces - 1)
        def _():
            for m in range(pieces):
                relay_copy(m).wait_recv()

            @pl.loop(0, line_size * chunks)
            def _(c):
                away = jnp.abs(c // chunks - line)
                arrived = rank((away - 1) * chunks + c % chunks)

                @pl.when((away == 0) | (arrived < pieces))
                def _():
                    work(c, 1, 2)

    @pl.loop(0, steps - 1)
    def _(step):
        take(step)

    def return_terms(near):
        for hop in range(1, line_size):
            other = (line + hop) % line_size
            away = jnp.abs(other - line)

            @pl.when((away == 1) if near else (away > 1))
            def _():
                theirs = pl.ds(other * chunks, chunks)
                ingest_sums[theirs] = jnp.sum(by_ingest[theirs], axis=1, keepdims=True)
                term_copy(other).start()

    early = pieces < steps
    if early:
        return_terms(False)
    take(steps - 1)
    if not early:
        return_terms(False)
    return_terms(True)
    mine = pl.ds(line * chunks, chunks)
    ingest_sums[mine] = jnp.sum(by_ingest[mine], axis=1, keepdims=True)

    def gather_slot(slot):
        block = by_resident[slot * held:(slot + 1) * held, :]
        resident_sums[slot] = jnp.sum(block.T, axis=0, keepdims=True)

    gather_slot(3)
    gather_slot(2)
    part_copy(3).start()
    gather_slot(1)
    part_copy(2).start()
    gather_slot(0)
    part_copy(1).start()

    for c in range(line_size * chunks):
        @pl.when((c // chunks <= line) & (line + 1 < line_size))
        def _():
            for copy in up_copies(c):
                copy.wait_send()

        @pl.when((c // chunks >= line) & (line > 0))
        def _():
            for copy in down_copies(c):
                copy.wait_send()
    for m in range(pieces):
        peer_copy(m).wait_send()
        relay_copy(m).wait_send()
    core_copy.wait_send()

    resident_total = resident_sums[0]
    for slot in (1, 2, 3):
        part_copy(slot).wait()
        resident_total = resident_total + resident_terms[slot]
    resident_out[...] = resident_total
    ingest_total = ingest_sums[mine]
    for hop in range(1, line_size):
        other = (line + hop) % line_size
        term_arrival(other).wait_recv()
        ingest_total = ingest_total + ingest_terms[pl.ds(other * chunks, chunks)]
    ingest_out[...] = ingest_total
    for hop in range(1, line_size):
        other = (line + hop) % line_size
        term_copy(other).wait_send()


def score_kernel(resident_total, ingest_total, resident_score, ingest_score):
    resident_score[...] = jnp.log1p(resident_total[...])
    ingest_score[...] = jnp.log1p(ingest_total[...])


def dense_on_device(cycle, resident, ingest, cluster_ids):
    held, columns = resident.shape
    count = ingest.shape[0]
    chunks = count // INGEST_CHUNK
    blocks = cycle // PAIR * chunks
    line_size = cycle // PAIR
    pieces = held // RESIDENT_CHUNK
    dma = pltpu.SemaphoreType.DMA
    vmem = pl.BlockSpec(memory_space=pltpu.VMEM)
    resident_total, ingest_total = pl.pallas_call(
        functools.partial(dense_kernel, cycle),
        out_shape=(
            jax.ShapeDtypeStruct((1, held), jnp.float32),
            jax.ShapeDtypeStruct((chunks, 1, INGEST_CHUNK), jnp.float32),
        ),
        in_specs=[pl.BlockSpec(memory_space=pl.ANY)] * 3,
        out_specs=(vmem, vmem),
        scratch_shapes=[
            pltpu.VMEM((count, columns), jnp.bfloat16),
            pltpu.VMEM((held, columns), jnp.bfloat16),
            dma((3,)),
            pltpu.VMEM((blocks, INGEST_CHUNK, columns), jnp.bfloat16),
            pltpu.VMEM((4 * held, columns), jnp.bfloat16),
            pltpu.VMEM((blocks, 1, INGEST_CHUNK), jnp.int32),
            pltpu.VMEM((4 * held, LANES), jnp.float32),
            pltpu.VMEM((blocks, SUBLANES, INGEST_CHUNK), jnp.float32),
            pltpu.VMEM((4, 1, held), jnp.float32),
            pltpu.VMEM((blocks, 1, INGEST_CHUNK), jnp.float32),
            pltpu.VMEM((4, 1, held), jnp.float32),
            pltpu.VMEM((blocks, 1, INGEST_CHUNK), jnp.float32),
            dma((blocks, HALVES)), dma((blocks, HALVES)), dma((blocks, HALVES)),
            dma((blocks,)), dma((blocks,)), dma((blocks,)),
            dma((pieces,)), dma((pieces,)),
            dma, dma,
            dma((pieces,)), dma((pieces,)),
            dma((4,)), dma((4,)),
            dma((line_size,)), dma((line_size,)),
        ],
        compiler_params=pltpu.CompilerParams(collective_id=0, has_side_effects=True),
    )(cluster_ids.reshape(chunks, 1, INGEST_CHUNK), ingest, resident)
    resident_score, ingest_score = pl.pallas_call(
        score_kernel,
        out_shape=(
            jax.ShapeDtypeStruct(resident_total.shape, jnp.float32),
            jax.ShapeDtypeStruct(ingest_total.shape, jnp.float32),
        ),
        in_specs=[vmem] * 2,
        out_specs=(vmem, vmem),
    )(resident_total, ingest_total)
    return (resident_score.reshape(held), ingest_score.reshape(count))


def solution(mesh):
    in_specs = (
        P(("groups", "blk", "rep"), None),
        P(("groups", "blk", "rep"), None),
        P(("groups", "blk", "rep")),
    )
    out_specs = (P(("groups", "blk", "rep")), P(("groups", "blk", "rep")))
    cycle = mesh.shape["blk"]
    dense = 2 * (CYCLE_STEPS + 1) >= cycle and cycle % PAIR == 0 and mesh.shape["rep"] == 2
    body = functools.partial(dense_on_device, cycle) if dense else on_device
    return jax.shard_map(
        body, mesh=mesh, in_specs=in_specs, out_specs=out_specs, check_vma=False
    )
```

```python
import functools
import math

import jax
import jax.numpy as jnp
from jax import lax
from jax.experimental import pallas as pl
from jax.experimental.pallas import tpu as pltpu
from jax.sharding import PartitionSpec as P

INGEST_DEV = 512
CL_OWN = 16
CYCLE_STEPS = 4


temper = 0.2
epsilon = 1e-06


def shifted(value, axis, steps):
    count = lax.axis_size(axis)
    pairs = [(source, (source + steps) % count) for source in range(count)]
    return lax.ppermute(value, axis, pairs)


def unit_rows(rows):
    values = rows.astype(jnp.float32)
    squares = jnp.sum(values * values, axis=-1, keepdims=True) + epsilon
    factor = lax.rsqrt(squares)
    return (values * factor).astype(jnp.bfloat16)


def kernel_sums(visitors, occupancy, residents):
    count_rows = visitors.shape[0]
    block_rows = 512
    num_blocks = count_rows // block_rows
    visit_blocks = visitors.reshape(num_blocks, block_rows, visitors.shape[1])
    live_blocks = occupancy.astype(jnp.float32).reshape(num_blocks, block_rows)

    def tile_sums(running, pieces):
        visit_tile, live_tile = pieces
        scores = jnp.einsum("vd,rd->vr", visit_tile, residents, preferred_element_type=jnp.float32)
        kernel = jnp.exp((scores - 1.0) / temper)
        return (running + jnp.sum(kernel * live_tile[:, None], axis=0), jnp.sum(kernel, axis=1))

    resident_part, visit_parts = lax.scan(
        tile_sums, jnp.zeros((residents.shape[0],), jnp.float32), (visit_blocks, live_blocks)
    )
    return (visit_parts.reshape(count_rows), resident_part)


def on_device(resident, ingest, cluster_ids):
    cycle_size = lax.axis_size("blk")
    slot_count = 3 * INGEST_DEV // (2 * cycle_size)
    columns = ingest.shape[1]
    owners = cluster_ids // CL_OWN
    onehot = (owners[:, None] == jnp.arange(cycle_size, dtype=jnp.int32)[None, :]).astype(jnp.int32)
    rank_within = jnp.sum((jnp.cumsum(onehot, axis=0) - onehot) * onehot, axis=1)
    targets = owners * slot_count + rank_within
    unit_ingest = unit_rows(ingest)
    outgoing = (
        jnp.zeros((cycle_size * slot_count, columns), jnp.bfloat16).at[targets].set(unit_ingest)
    )
    filled = (
        jnp.zeros((cycle_size * slot_count,), jnp.bfloat16)
        .at[targets]
        .set(jnp.ones((ingest.shape[0],), jnp.bfloat16))
    )
    arrived, present = (
        lax.all_to_all(
            outgoing.reshape(cycle_size, slot_count, columns),
            "blk",
            split_axis=0,
            concat_axis=0,
            tiled=True,
        ),
        lax.all_to_all(
            filled.reshape(cycle_size, slot_count), "blk", split_axis=0, concat_axis=0, tiled=True
        ),
    )
    visitors, marked = (
        lax.all_gather(
            arrived.reshape(cycle_size * slot_count, columns), "rep", axis=0, tiled=True
        ),
        lax.all_gather(present.reshape(cycle_size * slot_count), "rep", axis=0, tiled=True),
    )
    unit_resident = unit_rows(resident)
    visit_total = jnp.zeros((visitors.shape[0],), jnp.float32)
    resident_total = jnp.zeros((resident.shape[0],), jnp.float32)
    moving = unit_resident
    for rotation in range(CYCLE_STEPS + 1):
        if rotation > 0:
            moving = shifted(moving, "blk", -1)
            resident_total = shifted(resident_total, "blk", -1)
        visit_part, resident_part = kernel_sums(visitors, marked, moving)
        visit_total = visit_total + visit_part
        resident_total = resident_total + resident_part
    resident_total = shifted(resident_total, "blk", CYCLE_STEPS)
    own_sums = lax.psum_scatter(visit_total, "rep", scatter_dimension=0, tiled=True)
    returned = lax.all_to_all(
        own_sums.reshape(cycle_size, slot_count), "blk", split_axis=0, concat_axis=0, tiled=True
    )
    density = returned.reshape(cycle_size * slot_count)[targets]
    return (jnp.log1p(resident_total), jnp.log1p(density))


PAIR = 2
LANES = 128
SUBLANES = 8
INGEST_CHUNK = 256
RESIDENT_CHUNK = 256
HALVES = 2
LINE = 4
SUBS = 8
MESH = pl.DeviceIdType.MESH


def dense_kernel(
    cycle, ids_ref, ingest_ref, resident_ref, resident_out, ingest_out,
    raw_ingest, raw_resident, load_sem, rows, bank, ids, by_resident, by_ingest, resident_sums, ingest_sums, resident_terms, ingest_terms,
    up_send, down_send, rows_recv, up_ids_send, down_ids_send, ids_recv, peer_send, peer_recv, core_send, core_recv,
    relay_send, relay_recv, part_send, part_recv, term_send, term_recv,
):
    line_size = cycle // PAIR
    me = lax.axis_index("blk")
    core = lax.axis_index("rep")
    line, side = me // PAIR, me % PAIR
    chunks = ingest_ref.shape[0] // INGEST_CHUNK
    held = resident_ref.shape[0]
    pieces = held // RESIDENT_CHUNK
    tile_rows = 2 * held
    steps = (line_size - 1) * chunks
    half_rows = INGEST_CHUNK // HALVES
    at_end = (line == 0) | (line == line_size - 1)
    below_end, above_end = line == 1, line == line_size - 2
    holds_back = line_size > 2

    def device(at_line, at_side, at_core):
        return {"blk": at_line * PAIR + at_side, "rep": at_core}

    sibling = device(line, side, 1 - core)
    peer = device(line, 1 - side, core)
    across = device(line, 1 - side, 1 - core)

    def remote(source, target, send, recv, where):
        return pltpu.make_async_remote_copy(
            src_ref=source, dst_ref=target, send_sem=send, recv_sem=recv, device_id=where, device_id_type=MESH
        )

    def row_copy(c, h, send, where):
        part = rows.at[c, pl.ds(h * half_rows, half_rows)]
        return remote(part, part, send.at[c, h], rows_recv.at[c, h], where)

    def id_copy(c, send, where):
        return remote(ids.at[c], ids.at[c], send.at[c], ids_recv.at[c], where)

    above, below = device(line + 1, side, core), device(line - 1, side, core)

    def up_copies(c):
        return [id_copy(c, up_ids_send, above)] + [row_copy(c, h, up_send, above) for h in range(HALVES)]

    def down_copies(c):
        return [id_copy(c, down_ids_send, below)] + [row_copy(c, h, down_send, below) for h in range(HALVES)]

    def start_all(copies):
        for copy in copies:
            copy.start()

    def peer_copy(m):
        return remote(
            bank.at[pl.ds(m * RESIDENT_CHUNK, RESIDENT_CHUNK)],
            bank.at[pl.ds(2 * held + m * RESIDENT_CHUNK, RESIDENT_CHUNK)],
            peer_send.at[m], peer_recv.at[m], peer,
        )

    def relay_copy(m):
        return remote(
            bank.at[pl.ds(2 * held + m * RESIDENT_CHUNK, RESIDENT_CHUNK)],
            bank.at[pl.ds(3 * held + m * RESIDENT_CHUNK, RESIDENT_CHUNK)],
            relay_send.at[m], relay_recv.at[m], sibling,
        )

    core_copy = remote(bank.at[pl.ds(0, held)], bank.at[pl.ds(held, held)], core_send, core_recv, sibling)

    def term_copy(other):
        return remote(
            ingest_sums.at[pl.ds(other * chunks, chunks)], ingest_terms.at[pl.ds(line * chunks, chunks)],
            term_send.at[other], term_recv.at[line], device(other, side, core),
        )

    def term_arrival(other):
        return remote(
            ingest_sums.at[pl.ds(other * chunks, chunks)], ingest_terms.at[pl.ds(other * chunks, chunks)],
            term_send.at[other], term_recv.at[other], device(other, side, core),
        )

    def part_copy(slot):
        return remote(
            resident_sums.at[slot], resident_terms.at[slot], part_send.at[slot], part_recv.at[slot],
            (None, sibling, peer, across)[slot],
        )

    barrier = pltpu.get_barrier_semaphore()
    for where in (sibling, peer, across):
        pl.semaphore_signal(barrier, inc=1, device_id=where, device_id_type=MESH)

    @pl.when(line > 0)
    def _():
        pl.semaphore_signal(barrier, inc=1, device_id=below, device_id_type=MESH)

    @pl.when(line + 1 < line_size)
    def _():
        pl.semaphore_signal(barrier, inc=1, device_id=above, device_id_type=MESH)

    ingest_load = pltpu.make_async_copy(ingest_ref, raw_ingest, load_sem.at[0])
    resident_load = pltpu.make_async_copy(resident_ref, raw_resident, load_sem.at[1])
    ids_load = pltpu.make_async_copy(ids_ref, ids.at[pl.ds(line * chunks, chunks)], load_sem.at[2])
    for load in (ingest_load, ids_load, resident_load):
        load.start()

    def unit(block):
        values = block.astype(jnp.float32)
        squares = jnp.sum(values * values, axis=-1, keepdims=True) + epsilon
        return (values * lax.rsqrt(squares)).astype(jnp.bfloat16)

    ingest_load.wait()
    for j in range(chunks):
        rows[line * chunks + j] = unit(raw_ingest[j * INGEST_CHUNK:(j + 1) * INGEST_CHUNK, :])
    ids_load.wait()
    pl.semaphore_wait(barrier, 3 + (line > 0).astype(jnp.int32) + (line + 1 < line_size).astype(jnp.int32))
    for j in range(chunks):
        kept = holds_back and j == chunks - 1

        @pl.when((line + 1 < line_size) & jnp.logical_not(above_end & kept))
        def _():
            start_all(up_copies(line * chunks + j))

        @pl.when((line > 0) & jnp.logical_not(below_end & kept))
        def _():
            start_all(down_copies(line * chunks + j))

    resident_load.wait()

    @pl.loop(0, pieces)
    def _(m):
        part = pl.ds(m * RESIDENT_CHUNK, RESIDENT_CHUNK)
        bank[part, :] = unit(raw_resident[part, :])

    for m in range(pieces):
        peer_copy(m).start()
    core_copy.start()
    by_resident[...] = jnp.zeros_like(by_resident)
    by_ingest[...] = jnp.zeros_like(by_ingest)

    scale = math.log2(math.e) / temper
    span = CL_OWN * cycle

    def work(c, first, last):
        @pl.loop(first, last)
        def _(tile):
            part = pl.ds(pl.multiple_of(tile * tile_rows, tile_rows), tile_rows)
            position = line * PAIR + jnp.where(tile == 0, side, 1 - side)
            gap = (position + 1) * CL_OWN - 1 - ids[c]
            gap = jnp.where(gap < 0, gap + span, gap)
            bias = jnp.where(gap < CL_OWN * (CYCLE_STEPS + 1), -scale, -1e30)
            scores = lax.dot_general(
                bank[part, :], rows[c], (((1,), (1,)), ((), ())), preferred_element_type=jnp.float32
            )
            kernel = jnp.exp2(scores * scale + bias)
            by_ingest[c] += jnp.sum(kernel.reshape(tile_rows // SUBLANES, SUBLANES, INGEST_CHUNK), axis=0)
            folded = kernel[:, :LANES]
            for n in range(1, INGEST_CHUNK // LANES):
                folded = folded + kernel[:, n * LANES:(n + 1) * LANES]
            by_resident[part, :] += folded

    core_copy.wait_recv()

    @pl.loop(0, chunks)
    def _(j):
        work(line * chunks + j, 0, 1)

    def place(step):
        if not holds_back:
            return step
        turned = jnp.where(step == 0, 0, step + chunks - 1)
        late = step >= steps - chunks + 1
        return jnp.where(at_end & (chunks > 1), jnp.where(late, step - (steps - chunks), turned), step)

    def rank(spot):
        if not holds_back:
            return spot
        turned = jnp.where(spot == 0, 0, spot - chunks + 1)
        late = (spot >= 1) & (spot < chunks)
        return jnp.where(at_end & (chunks > 1), jnp.where(late, spot + steps - chunks, turned), spot)

    def take(step):
        spot = place(step)
        hop, j = spot // chunks + 1, spot % chunks

        @pl.when(line - hop >= 0)
        def _():
            for copy in up_copies((line - hop) * chunks + j):
                copy.wait_recv()

                @pl.when(line + 1 < line_size)
                def _():
                    copy.start()

        @pl.when(line + hop < line_size)
        def _():
            for copy in down_copies((line + hop) * chunks + j):
                copy.wait_recv()

                @pl.when(line > 0)
                def _():
                    copy.start()

        if holds_back:
            @pl.when((step == (line_size - 2) * chunks - 1) & above_end)
            def _():
                start_all(up_copies(line * chunks + chunks - 1))

            @pl.when((step == (line_size - 2) * chunks - 1) & below_end)
            def _():
                start_all(down_copies(line * chunks + chunks - 1))

        @pl.when(step < pieces)
        def _():
            peer_copy(step).wait_recv()
            relay_copy(step).start()

        @pl.loop(0, 2)
        def _(way):
            other = line + (2 * way - 1) * hop

            @pl.when((other >= 0) & (other < line_size))
            def _():
                work(other * chunks + j, 0, jnp.where(step < pieces, 1, 2))

        @pl.when(step == pieces - 1)
        def _():
            for m in range(pieces):
                relay_copy(m).wait_recv()

            @pl.loop(0, line_size * chunks)
            def _(c):
                away = jnp.abs(c // chunks - line)
                arrived = rank((away - 1) * chunks + c % chunks)

                @pl.when((away == 0) | (arrived < pieces))
                def _():
                    work(c, 1, 2)

    @pl.loop(0, steps - 1)
    def _(step):
        take(step)

    def return_terms(near):
        for hop in range(1, line_size):
            other = (line + hop) % line_size
            away = jnp.abs(other - line)

            @pl.when((away == 1) if near else (away > 1))
            def _():
                theirs = pl.ds(other * chunks, chunks)
                ingest_sums[theirs] = jnp.sum(by_ingest[theirs], axis=1, keepdims=True)
                term_copy(other).start()

    early = pieces < steps
    if early:
        return_terms(False)
    take(steps - 1)
    if not early:
        return_terms(False)
    return_terms(True)
    mine = pl.ds(line * chunks, chunks)
    ingest_sums[mine] = jnp.sum(by_ingest[mine], axis=1, keepdims=True)

    def gather_slot(slot):
        block = by_resident[slot * held:(slot + 1) * held, :]
        resident_sums[slot] = jnp.sum(block.T, axis=0, keepdims=True)

    gather_slot(3)
    gather_slot(2)
    part_copy(3).start()
    gather_slot(1)
    part_copy(2).start()
    gather_slot(0)
    part_copy(1).start()

    for c in range(line_size * chunks):
        @pl.when((c // chunks <= line) & (line + 1 < line_size))
        def _():
            for copy in up_copies(c):
                copy.wait_send()

        @pl.when((c // chunks >= line) & (line > 0))
        def _():
            for copy in down_copies(c):
                copy.wait_send()
    for m in range(pieces):
        peer_copy(m).wait_send()
        relay_copy(m).wait_send()
    core_copy.wait_send()

    resident_total = resident_sums[0]
    for slot in (1, 2, 3):
        part_copy(slot).wait()
        resident_total = resident_total + resident_terms[slot]
    resident_out[...] = resident_total
    ingest_total = ingest_sums[mine]
    for hop in range(1, line_size):
        other = (line + hop) % line_size
        term_arrival(other).wait_recv()
        ingest_total = ingest_total + ingest_terms[pl.ds(other * chunks, chunks)]
    ingest_out[...] = ingest_total
    for hop in range(1, line_size):
        other = (line + hop) % line_size
        term_copy(other).wait_send()


def score_kernel(resident_total, ingest_total, resident_score, ingest_score):
    resident_score[...] = jnp.log1p(resident_total[...])
    ingest_score[...] = jnp.log1p(ingest_total[...])


def scores_of(resident_total, ingest_total, held, count):
    vmem = pl.BlockSpec(memory_space=pltpu.VMEM)
    resident_score, ingest_score = pl.pallas_call(
        score_kernel,
        out_shape=(
            jax.ShapeDtypeStruct(resident_total.shape, jnp.float32),
            jax.ShapeDtypeStruct(ingest_total.shape, jnp.float32),
        ),
        in_specs=[vmem] * 2,
        out_specs=(vmem, vmem),
    )(resident_total, ingest_total)
    return (resident_score.reshape(held), ingest_score.reshape(count))


def dense_on_device(cycle, resident, ingest, cluster_ids):
    held, columns = resident.shape
    count = ingest.shape[0]
    chunks = count // INGEST_CHUNK
    blocks = cycle // PAIR * chunks
    line_size = cycle // PAIR
    pieces = held // RESIDENT_CHUNK
    dma = pltpu.SemaphoreType.DMA
    vmem = pl.BlockSpec(memory_space=pltpu.VMEM)
    resident_total, ingest_total = pl.pallas_call(
        functools.partial(dense_kernel, cycle),
        out_shape=(
            jax.ShapeDtypeStruct((1, held), jnp.float32),
            jax.ShapeDtypeStruct((chunks, 1, INGEST_CHUNK), jnp.float32),
        ),
        in_specs=[pl.BlockSpec(memory_space=pl.ANY)] * 3,
        out_specs=(vmem, vmem),
        scratch_shapes=[
            pltpu.VMEM((count, columns), jnp.bfloat16),
            pltpu.VMEM((held, columns), jnp.bfloat16),
            dma((3,)),
            pltpu.VMEM((blocks, INGEST_CHUNK, columns), jnp.bfloat16),
            pltpu.VMEM((4 * held, columns), jnp.bfloat16),
            pltpu.VMEM((blocks, 1, INGEST_CHUNK), jnp.int32),
            pltpu.VMEM((4 * held, LANES), jnp.float32),
            pltpu.VMEM((blocks, SUBLANES, INGEST_CHUNK), jnp.float32),
            pltpu.VMEM((4, 1, held), jnp.float32),
            pltpu.VMEM((blocks, 1, INGEST_CHUNK), jnp.float32),
            pltpu.VMEM((4, 1, held), jnp.float32),
            pltpu.VMEM((blocks, 1, INGEST_CHUNK), jnp.float32),
            dma((blocks, HALVES)), dma((blocks, HALVES)), dma((blocks, HALVES)),
            dma((blocks,)), dma((blocks,)), dma((blocks,)),
            dma((pieces,)), dma((pieces,)),
            dma, dma,
            dma((pieces,)), dma((pieces,)),
            dma((4,)), dma((4,)),
            dma((line_size,)), dma((line_size,)),
        ],
        compiler_params=pltpu.CompilerParams(collective_id=0, has_side_effects=True),
    )(cluster_ids.reshape(chunks, 1, INGEST_CHUNK), ingest, resident)
    return scores_of(resident_total, ingest_total, held, count)


def relay_kernel(
    cycle, ids_ref, ingest_ref, resident_ref, resident_out, ingest_out,
    raw_ingest, raw_resident, rows, guest, bank, ids, by_resident, by_ingest, resident_sums, ingest_sums,
    resident_terms, ingest_terms,
    load_sem, up_send, down_send, rows_recv, up_ids_send, down_ids_send, ids_recv,
    guest_send, guest_recv, guest_pass, out_send, out_recv, out_pass, direct_send, far_recv,
    peer_send, peer_recv, turn_send, turn_recv, turn_pass, cross_send, core_send, core_recv,
    near_send, near_recv, away_send, away_recv, part_send, part_recv, term_send, term_recv,
):
    group = lax.axis_index("groups")
    me = lax.axis_index("blk")
    core = lax.axis_index("rep")
    level, side = me // PAIR, me % PAIR
    role = jnp.where(group == 0, level, LINE - 1 - level)
    count, held = ingest_ref.shape[0], resident_ref.shape[0]
    chunk, half = count // 2, count // 4
    sub = held // SUBS
    quad = held // 2

    def level_of(at_role, at_group):
        return jnp.where(at_group == 0, at_role, LINE - 1 - at_role)

    def device(at_role, at_side, at_core):
        return {"groups": group, "blk": level_of(at_role, group) * PAIR + at_side, "rep": at_core}

    def other(at_role, at_side):
        return {"groups": 1 - group, "blk": level_of(at_role, 1 - group) * PAIR + at_side, "rep": core}

    sibling = device(role, side, 1 - core)
    peer = device(role, 1 - side, core)
    across = device(role, 1 - side, 1 - core)
    above, below = device(role + 1, side, core), device(role - 1, side, core)

    def remote(source, target, send, recv, where):
        return pltpu.make_async_remote_copy(
            src_ref=source, dst_ref=target, send_sem=send, recv_sem=recv, device_id=where, device_id_type=MESH
        )

    def got(target, recv):
        remote(target, target, core_send, recv, sibling).wait_recv()

    def part(c, h):
        return rows.at[pl.ds(c * chunk + h * half, half)]

    def strip(start, size):
        return bank.at[pl.ds(start, size)]

    def own_at(r):
        return r * sub

    def peer_at(r, theirs=0):
        return 2 * held + (r // 4) * held + (r % 4) * sub + theirs * quad

    def far_at(line, r, theirs=0):
        if line == 0:
            return 4 * held + (r // 4) * held + (r % 4) * sub + theirs * quad
        if r < 4:
            return 6 * held + r * sub + theirs * quad
        return 7 * held + (r - 4) // 2 * quad + (r % 2) * sub + theirs * (quad // 2)

    def up(c, h):
        return remote(part(c, h), part(c, h), up_send.at[c, h], rows_recv.at[c, h], above)

    def down(c, h):
        return remote(part(c, h), part(c, h), down_send.at[c, h], rows_recv.at[c, h], below)

    def up_ids(c):
        return remote(ids.at[c], ids.at[c], up_ids_send.at[c], ids_recv.at[c], above)

    def down_ids(c):
        return remote(ids.at[c], ids.at[c], down_ids_send.at[c], ids_recv.at[c], below)

    def guest_part(h):
        return guest.at[pl.ds(h * half, half)]

    def guest_copy(h):
        return remote(part(3, h), guest_part(h), guest_send.at[h], guest_recv.at[h], other(2, side))

    def guest_on(h):
        return remote(guest_part(h), part(3, h), guest_pass.at[h], rows_recv.at[3, h], other(0, side))

    def out_spot(i):
        return (0, i) if i < 4 else (1, i - 4)

    def out_copy(i):
        line, r = out_spot(i)
        source = own_at(r) if line == 0 else peer_at(r)
        return remote(
            strip(source, sub), strip(far_at(line, r), sub), out_send.at[i], out_recv.at[i], other(0, side)
        )

    def out_on(i):
        line, r = out_spot(i)
        spot = strip(far_at(line, r), sub)
        return remote(spot, spot, out_pass.at[i], far_recv.at[line, r], other(2, side))

    def direct_copy(i):
        line, r = (0, i + 4) if i < 4 else (1, i - 2)
        source = own_at(r) if line == 0 else peer_at(r)
        return remote(
            strip(source, sub), strip(far_at(line, r), sub), direct_send.at[i], far_recv.at[line, r], below
        )

    def peer_copy(r):
        return remote(strip(own_at(r), sub), strip(peer_at(r), sub), peer_send.at[r], peer_recv.at[r], peer)

    def turn_copy(k):
        r = k + 6
        return remote(
            strip(own_at(r), sub), strip(far_at(0, r), sub), turn_send.at[k], turn_recv.at[k], other(1, 1 - side)
        )

    def turn_on(k):
        r = k + 6
        return remote(
            strip(far_at(0, r), sub), strip(peer_at(r), sub), turn_pass.at[k], peer_recv.at[r], other(2, side)
        )

    def cross_copy(r):
        return remote(
            strip(far_at(0, r), sub), strip(far_at(1, r), sub), cross_send.at[r - 4], far_recv.at[1, r], peer
        )

    core_copy = remote(strip(0, held), strip(held, held), core_send, core_recv, sibling)

    def near_copy(r):
        return remote(strip(peer_at(r), sub), strip(peer_at(r, 1), sub), near_send.at[r], near_recv.at[r], sibling)

    def away_copy(line, r):
        return remote(
            strip(far_at(line, r), sub), strip(far_at(line, r, 1), sub),
            away_send.at[line, r], away_recv.at[line, r], sibling,
        )

    def term_copy(k):
        return remote(
            ingest_sums.at[pl.ds(2 * k, 2)], ingest_terms.at[role], term_send.at[k], term_recv.at[role],
            device(k, side, core),
        )

    def term_got(k):
        got(ingest_terms.at[k], term_recv.at[k])

    def part_copy(slot):
        if slot >= 4:
            where = device(3, side if slot < 6 else 1 - side, core if slot % 2 == 0 else 1 - core)
        else:
            where = (None, sibling, peer, across)[slot]
        return remote(resident_sums.at[slot], resident_terms.at[slot], part_send.at[slot], part_recv.at[slot], where)

    inner = (role == 1) | (role == 2)
    barrier = pltpu.get_barrier_semaphore()

    def greet(where):
        pl.semaphore_signal(barrier, inc=1, device_id=where, device_id_type=MESH)

    for where in (sibling, peer, across, other(LINE - 1 - role, side)):
        greet(where)
    pl.when(role > 0)(lambda: greet(below))
    pl.when(role < LINE - 1)(lambda: greet(above))
    pl.when(inner)(lambda: greet(other(LINE - 1 - role, 1 - side)))
    greeted = (
        4 + (role > 0).astype(jnp.int32) + (role < LINE - 1).astype(jnp.int32) + inner.astype(jnp.int32)
    )

    def ingest_load(s):
        piece = pl.ds(s * half, half)
        return pltpu.make_async_copy(ingest_ref.at[piece], raw_ingest.at[piece], load_sem.at[s])

    def resident_load(m):
        piece = pl.ds(m * 2 * sub, 2 * sub)
        return pltpu.make_async_copy(resident_ref.at[piece], raw_resident.at[piece], load_sem.at[4 + m])

    ids_load = pltpu.make_async_copy(ids_ref, ids.at[pl.ds(2 * role, 2)], load_sem.at[8])
    ingest_load(0).start()
    ids_load.start()
    for s in range(1, 4):
        ingest_load(s).start()
    for m in range(4):
        resident_load(m).start()

    def unit(block):
        values = block.astype(jnp.float32)
        squares = jnp.sum(values * values, axis=-1, keepdims=True) + epsilon
        return (values * lax.rsqrt(squares)).astype(jnp.bfloat16)

    def ready(s):
        ingest_load(s).wait()
        rows[pl.ds(role * count + s * half, half), :] = unit(raw_ingest[s * half:(s + 1) * half, :])

    ready(0)
    ids_load.wait()
    pl.semaphore_wait(barrier, greeted)
    for s in range(4):
        j, h = s // 2, s % 2
        if s:
            ready(s)
        c = 2 * role + j

        @pl.when((role == 1) | (role == 2) | ((role == 0) & (j == 0)))
        def _():
            up(c, h).start()

        @pl.when((role == 2) | ((role == 1) & (j == 0)) | ((role == 3) & (j == 0)))
        def _():
            down(c, h).start()

        if j == 1:
            @pl.when(role == 1)
            def _():
                guest_copy(h).start()
        if s == 0:
            for k in range(2):
                @pl.when(role < 3)
                def _():
                    up_ids(2 * role + k).start()

                @pl.when(role > 0)
                def _():
                    down_ids(2 * role + k).start()

    for m in range(4):
        resident_load(m).wait()
        piece = pl.ds(m * 2 * sub, 2 * sub)
        bank[piece, :] = unit(raw_resident[piece, :])
        for r in (2 * m, 2 * m + 1):
            @pl.when((role < 2) | ((role == 2) & (r < 6)) | ((role == 3) & (r < 4)))
            def _():
                peer_copy(r).start()

            if r >= 6:
                @pl.when(role == 2)
                def _():
                    turn_copy(r - 6).start()

            if r < 4:
                @pl.when(role == 3)
                def _():
                    out_copy(r).start()
            else:
                @pl.when(role == 3)
                def _():
                    direct_copy(r - 4).start()
            if r == 5:
                @pl.when(role == 3)
                def _():
                    down(7, 0).start()
                    down(7, 1).start()
    core_copy.start()
    by_resident[pl.ds(0, 4 * held), :] = jnp.zeros((4 * held, LANES), jnp.float32)
    by_ingest[...] = jnp.zeros_like(by_ingest)

    @pl.when(role == 2)
    def _():
        by_resident[pl.ds(4 * held, 4 * held), :] = jnp.zeros((4 * held, LANES), jnp.float32)

    scale = math.log2(math.e) / temper
    span = CL_OWN * cycle

    def work(c, start, size, position):
        spot = pl.ds(start, size)
        gap = (position + 1) * CL_OWN - 1 - ids[c]
        gap = jnp.where(gap < 0, gap + span, gap)
        bias = jnp.where(gap < CL_OWN * (CYCLE_STEPS + 1), -scale, -1e30)
        block = rows[pl.ds(pl.multiple_of(c * chunk, chunk), chunk), :]
        scores = lax.dot_general(bank[spot, :], block, (((1,), (1,)), ((), ())), preferred_element_type=jnp.float32)
        kernel = jnp.exp2(scores * scale + bias)
        by_ingest[c] += jnp.sum(kernel.reshape(size // SUBLANES, SUBLANES, chunk), axis=0)
        folded = kernel[:, :LANES]
        for n in range(1, chunk // LANES):
            folded = folded + kernel[:, n * LANES:(n + 1) * LANES]
        by_resident[spot, :] += folded

    here = level * PAIR + side
    beside = level * PAIR + 1 - side
    end = level_of(3, group) * PAIR
    home = (0, 2 * held, here)
    next0 = (2 * held, held, beside)
    next1 = (3 * held, held, beside)
    next_all = (2 * held, 2 * held, beside)
    far_all = (4 * held, 2 * held, end + side)
    far2 = (6 * held, held, end + 1 - side)
    far3 = (7 * held, quad, end + 1 - side)
    far4 = (7 * held + quad, quad, end + 1 - side)

    def do(first, last, *blocks):
        @pl.loop(first, last)
        def _(c):
            for block in blocks:
                work(c, *block)

    def take(c, h, *onward):
        got(part(c, h), rows_recv.at[c, h])
        if h == 0:
            got(ids.at[c], ids_recv.at[c])
        for way in onward:
            way(c, h).start()
            if h == 0:
                (up_ids if way is up else down_ids)(c).start()

    def meet(*subs):
        for r in subs:
            got(strip(peer_at(r), sub), peer_recv.at[r])
            near_copy(r).start()

    def met(*subs):
        for r in subs:
            got(strip(peer_at(r, 1), sub), near_recv.at[r])

    def reach(line, *subs):
        for r in subs:
            got(strip(far_at(line, r), sub), far_recv.at[line, r])
            if line == 0 and r >= 4:
                cross_copy(r).start()
            away_copy(line, r).start()

    def reached(line, *subs):
        for r in subs:
            got(strip(far_at(line, r, 1), sub), away_recv.at[line, r])

    def pass_out(i):
        line, r = out_spot(i)
        got(strip(far_at(line, r), sub), out_recv.at[i])
        out_on(i).start()

    core_copy.wait_recv()

    @pl.loop(0, 2)
    def _(j):
        work(2 * role + j, *home)

    @pl.when(role == 0)
    def _():
        pass_out(0)
        pass_out(1)
        up(1, 0).start()
        up(1, 1).start()
        take(2, 0)
        take(2, 1)
        meet(0, 1)
        do(2, 3, home)
        take(3, 0)
        take(3, 1)
        take(4, 0)
        pass_out(2)
        meet(2)
        take(4, 1)
        pass_out(3)
        meet(3)
        do(3, 5, home)
        met(0, 1, 2, 3)
        do(0, 5, next0)
        take(5, 0)
        meet(4)
        pass_out(4)
        take(5, 1)
        meet(5)
        pass_out(5)
        do(5, 6, home, next0)
        take(6, 0)
        meet(6)
        take(6, 1)
        meet(7)
        do(6, 7, home, next0)
        met(4, 5, 6, 7)
        do(0, 7, next1)
        take(7, 0)
        take(7, 1)
        do(7, 8, home, next_all)

    @pl.when(role == 1)
    def _():
        take(0, 0, up)
        take(4, 0, down)
        take(0, 1, up)
        take(4, 1, down)
        meet(0)
        do(0, 1, home)
        do(4, 5, home)
        take(5, 0, down)
        meet(1)
        take(5, 1, down)
        do(5, 6, home)
        for k in range(2):
            got(strip(far_at(0, k + 6), sub), turn_recv.at[k])
            turn_on(k).start()
        meet(2)
        take(1, 0, up)
        take(6, 0, down)
        meet(3)
        take(1, 1, up)
        take(6, 1, down)
        do(1, 2, home)
        do(6, 7, home)
        met(0, 1, 2, 3)
        do(0, 4, next0)
        take(7, 0, down)
        meet(4)
        do(4, 7, next0)
        take(7, 1, down)
        meet(5)
        do(7, 8, home, next0)
        meet(6, 7)
        met(4, 5, 6, 7)
        do(0, 8, next1)

    @pl.when(role == 2)
    def _():
        take(6, 0, down)
        for h in range(2):
            got(guest_part(h), guest_recv.at[h])
            guest_on(h).start()
            if h == 0:
                take(2, 0, up)
                take(6, 1, down)
        take(2, 1, up)
        meet(0, 1)
        do(2, 3, home)
        do(6, 7, home)
        take(3, 0, up)
        reach(0, 4)
        meet(2)
        take(3, 1, up)
        reach(0, 5)
        meet(3)
        do(3, 4, home)
        reach(0, 0, 1)
        met(0, 1, 2, 3)
        do(2, 5, next0)
        take(7, 0, down)
        do(5, 7, next0)
        take(7, 1, down)
        do(7, 8, home, next0)
        take(0, 0)
        take(0, 1)
        meet(4, 5, 6, 7)
        do(0, 1, home, next0)
        met(4, 5, 6, 7)
        do(2, 5, next1)
        reach(0, 6)
        do(5, 8, next1)
        take(1, 0)
        take(1, 1)
        do(0, 1, next1)
        reach(0, 7)
        do(1, 2, home, next_all)
        reach(1, 4, 5)
        reach(0, 2, 3)
        reached(0, 0, 1, 2, 3, 4, 5, 6, 7)
        do(0, 2, far_all)
        reached(1, 4, 5)
        do(0, 8, far3)
        reach(1, 2, 6, 0, 3, 7, 1)
        reached(1, 6, 7)
        do(0, 8, far4)
        reached(1, 0, 1, 2, 3)
        do(0, 2, far2)

    @pl.when(role == 3)
    def _():
        for r in range(2):
            meet(r)
            out_copy(4 + r).start()
        take(4, 0)
        take(4, 1)
        do(4, 5, home)
        for r in range(2, 4):
            meet(r)
            direct_copy(r + 2).start()
        met(0, 1, 2, 3)
        do(6, 8, next0)
        do(4, 5, next0)
        take(5, 0)
        take(5, 1)
        do(5, 6, home, next0)
        take(2, 0)
        take(2, 1)
        do(2, 3, home, next0)
        take(3, 0)
        take(3, 1)
        do(3, 4, home, next0)

    ingest_sums[...] = jnp.sum(by_ingest[...], axis=1, keepdims=True)
    for k in range(LINE):
        @pl.when((role != k) & ((role < 3) | (k > 0)))
        def _():
            term_copy(k).start()

    def gather(start, size):
        return jnp.sum(by_resident[start:start + size, :].T, axis=0, keepdims=True)

    def gather_pair(slot, first, second):
        resident_sums[slot, :, 0:quad] = gather(first, quad)
        resident_sums[slot, :, quad:held] = gather(second, quad)
        part_copy(slot).start()

    @pl.when(role == 2)
    def _():
        for slot in (6, 7):
            resident_sums[slot, :, 0:quad] = gather(far_at(1, 0, slot % 2), quad)
            for n in range(2):
                resident_sums[slot, :, quad + n * quad // 2:quad + (n + 1) * quad // 2] = gather(
                    far_at(1, 4 + 2 * n, slot % 2), quad // 2
                )
            part_copy(slot).start()
        for slot in (4, 5):
            gather_pair(slot, far_at(0, 0, slot % 2), far_at(0, 4, slot % 2))

    gather_pair(3, peer_at(0, 1), peer_at(4, 1))
    gather_pair(2, peer_at(0), peer_at(4))
    resident_sums[1] = gather(held, held)
    part_copy(1).start()
    resident_total = gather(0, held)

    for slot in (1, 2, 3):
        got(resident_terms.at[slot], part_recv.at[slot])
        resident_total = resident_total + resident_terms[slot]
    resident_out[...] = resident_total

    @pl.when(role == 3)
    def _():
        far_total = resident_out[...]
        for slot in (4, 5, 6, 7):
            got(resident_terms.at[slot], part_recv.at[slot])
            far_total = far_total + resident_terms[slot]
        resident_out[...] = far_total

    ingest_out[...] = ingest_sums[pl.ds(2 * role, 2)]
    for k in range(LINE):
        @pl.when((role != k) & ((k < 3) | (role > 0)))
        def _():
            term_got(k)
            ingest_out[...] += ingest_terms[k]

    for k in range(LINE):
        @pl.when((role != k) & ((role < 3) | (k > 0)))
        def _():
            term_copy(k).wait_send()
    for slot in (1, 2, 3):
        part_copy(slot).wait_send()
    core_copy.wait_send()

    def sent(condition, *copies):
        @pl.when(condition)
        def _():
            for copy in copies:
                copy().wait_send()

    def later(make, *arguments):
        return lambda: make(*arguments)

    pairs = [(c, h) for c in range(8) for h in range(2)]

    def flows(make, make_ids, chunks):
        return [later(make, c, h) for c, h in pairs if c in chunks] + [later(make_ids, c) for c in chunks]

    sent(
        role == 0,
        *flows(up, up_ids, (0, 1)), *[later(out_on, i) for i in range(6)],
        *[later(peer_copy, r) for r in range(8)], *[later(near_copy, r) for r in range(8)],
    )
    sent(
        role == 1,
        *flows(up, up_ids, (0, 1, 2, 3)), *flows(down, down_ids, (2, 4, 5, 6, 7)), later(down_ids, 3),
        *[later(guest_copy, h) for h in range(2)], *[later(turn_on, k) for k in range(2)],
        *[later(peer_copy, r) for r in range(8)], *[later(near_copy, r) for r in range(8)],
    )
    sent(
        role == 2,
        *flows(up, up_ids, (2, 3, 4, 5)), *flows(down, down_ids, (4, 5, 6, 7)),
        *[later(guest_on, h) for h in range(2)], *[later(turn_copy, k) for k in range(2)],
        *[later(peer_copy, r) for r in range(6)], *[later(near_copy, r) for r in range(8)],
        *[later(cross_copy, r) for r in range(4, 8)],
        *[later(away_copy, line, r) for line in range(2) for r in range(8)],
        *[later(part_copy, slot) for slot in (4, 5, 6, 7)],
    )
    sent(
        role == 3,
        *flows(down, down_ids, (6, 7)), *[later(out_copy, i) for i in range(6)],
        *[later(direct_copy, i) for i in range(6)],
        *[later(peer_copy, r) for r in range(4)], *[later(near_copy, r) for r in range(4)],
    )


def relay_on_device(cycle, resident, ingest, cluster_ids):
    held, columns = resident.shape
    count = ingest.shape[0]
    chunk = count // 2
    dma = pltpu.SemaphoreType.DMA
    vmem = pl.BlockSpec(memory_space=pltpu.VMEM)
    flows = dma((8, 2))
    eight = dma((8,))
    totals = pl.pallas_call(
        functools.partial(relay_kernel, cycle),
        out_shape=(
            jax.ShapeDtypeStruct((1, held), jnp.float32),
            jax.ShapeDtypeStruct((2, 1, chunk), jnp.float32),
        ),
        in_specs=[pl.BlockSpec(memory_space=pl.ANY)] * 3,
        out_specs=(vmem, vmem),
        scratch_shapes=[
            pltpu.VMEM((count, columns), jnp.bfloat16),
            pltpu.VMEM((held, columns), jnp.bfloat16),
            pltpu.VMEM((LINE * count, columns), jnp.bfloat16),
            pltpu.VMEM((chunk, columns), jnp.bfloat16),
            pltpu.VMEM((8 * held, columns), jnp.bfloat16),
            pltpu.VMEM((2 * LINE, 1, chunk), jnp.int32),
            pltpu.VMEM((8 * held, LANES), jnp.float32),
            pltpu.VMEM((2 * LINE, SUBLANES, chunk), jnp.float32),
            pltpu.VMEM((8, 1, held), jnp.float32),
            pltpu.VMEM((2 * LINE, 1, chunk), jnp.float32),
            pltpu.VMEM((8, 1, held), jnp.float32),
            pltpu.VMEM((LINE, 2, 1, chunk), jnp.float32),
            dma((9,)), flows, flows, flows, eight, eight, eight,
            dma((2,)), dma((2,)), dma((2,)), dma((6,)), dma((6,)), dma((6,)), dma((6,)), dma((2, 8)),
            eight, eight, dma((2,)), dma((2,)), dma((2,)), dma((4,)), dma, dma,
            eight, eight, dma((2, 8)), dma((2, 8)), eight, eight, dma((LINE,)), dma((LINE,)),
        ],
        compiler_params=pltpu.CompilerParams(collective_id=0, has_side_effects=True),
    )(cluster_ids.reshape(2, 1, chunk), ingest, resident)
    return scores_of(*totals, held, count)


def solution(mesh):
    in_specs = (
        P(("groups", "blk", "rep"), None),
        P(("groups", "blk", "rep"), None),
        P(("groups", "blk", "rep")),
    )
    out_specs = (P(("groups", "blk", "rep")), P(("groups", "blk", "rep")))
    cycle = mesh.shape["blk"]
    dense = 2 * (CYCLE_STEPS + 1) >= cycle and cycle % PAIR == 0 and mesh.shape["rep"] == 2
    body = functools.partial(dense_on_device, cycle) if dense else on_device
    if dense and cycle == LINE * PAIR and mesh.shape["groups"] == 2:
        body = functools.partial(relay_on_device, cycle)
    return jax.shard_map(
        body, mesh=mesh, in_specs=in_specs, out_specs=out_specs, check_vma=False
    )
```

```python
import functools
import math

import jax
import jax.numpy as jnp
from jax import lax
from jax.experimental import pallas as pl
from jax.experimental.pallas import tpu as pltpu
from jax.sharding import PartitionSpec as P

INGEST_DEV = 512
CL_OWN = 16
CYCLE_STEPS = 4


temper = 0.2
epsilon = 1e-06


def shifted(value, axis, steps):
    count = lax.axis_size(axis)
    pairs = [(source, (source + steps) % count) for source in range(count)]
    return lax.ppermute(value, axis, pairs)


def unit_rows(rows):
    values = rows.astype(jnp.float32)
    squares = jnp.sum(values * values, axis=-1, keepdims=True) + epsilon
    factor = lax.rsqrt(squares)
    return (values * factor).astype(jnp.bfloat16)


def kernel_sums(visitors, occupancy, residents):
    count_rows = visitors.shape[0]
    block_rows = 512
    num_blocks = count_rows // block_rows
    visit_blocks = visitors.reshape(num_blocks, block_rows, visitors.shape[1])
    live_blocks = occupancy.astype(jnp.float32).reshape(num_blocks, block_rows)

    def tile_sums(running, pieces):
        visit_tile, live_tile = pieces
        scores = jnp.einsum("vd,rd->vr", visit_tile, residents, preferred_element_type=jnp.float32)
        kernel = jnp.exp((scores - 1.0) / temper)
        return (running + jnp.sum(kernel * live_tile[:, None], axis=0), jnp.sum(kernel, axis=1))

    resident_part, visit_parts = lax.scan(
        tile_sums, jnp.zeros((residents.shape[0],), jnp.float32), (visit_blocks, live_blocks)
    )
    return (visit_parts.reshape(count_rows), resident_part)


def on_device(resident, ingest, cluster_ids):
    cycle_size = lax.axis_size("blk")
    slot_count = 3 * INGEST_DEV // (2 * cycle_size)
    columns = ingest.shape[1]
    owners = cluster_ids // CL_OWN
    onehot = (owners[:, None] == jnp.arange(cycle_size, dtype=jnp.int32)[None, :]).astype(jnp.int32)
    rank_within = jnp.sum((jnp.cumsum(onehot, axis=0) - onehot) * onehot, axis=1)
    targets = owners * slot_count + rank_within
    unit_ingest = unit_rows(ingest)
    outgoing = (
        jnp.zeros((cycle_size * slot_count, columns), jnp.bfloat16).at[targets].set(unit_ingest)
    )
    filled = (
        jnp.zeros((cycle_size * slot_count,), jnp.bfloat16)
        .at[targets]
        .set(jnp.ones((ingest.shape[0],), jnp.bfloat16))
    )
    arrived, present = (
        lax.all_to_all(
            outgoing.reshape(cycle_size, slot_count, columns),
            "blk",
            split_axis=0,
            concat_axis=0,
            tiled=True,
        ),
        lax.all_to_all(
            filled.reshape(cycle_size, slot_count), "blk", split_axis=0, concat_axis=0, tiled=True
        ),
    )
    visitors, marked = (
        lax.all_gather(
            arrived.reshape(cycle_size * slot_count, columns), "rep", axis=0, tiled=True
        ),
        lax.all_gather(present.reshape(cycle_size * slot_count), "rep", axis=0, tiled=True),
    )
    unit_resident = unit_rows(resident)
    visit_total = jnp.zeros((visitors.shape[0],), jnp.float32)
    resident_total = jnp.zeros((resident.shape[0],), jnp.float32)
    moving = unit_resident
    for rotation in range(CYCLE_STEPS + 1):
        if rotation > 0:
            moving = shifted(moving, "blk", -1)
            resident_total = shifted(resident_total, "blk", -1)
        visit_part, resident_part = kernel_sums(visitors, marked, moving)
        visit_total = visit_total + visit_part
        resident_total = resident_total + resident_part
    resident_total = shifted(resident_total, "blk", CYCLE_STEPS)
    own_sums = lax.psum_scatter(visit_total, "rep", scatter_dimension=0, tiled=True)
    returned = lax.all_to_all(
        own_sums.reshape(cycle_size, slot_count), "blk", split_axis=0, concat_axis=0, tiled=True
    )
    density = returned.reshape(cycle_size * slot_count)[targets]
    return (jnp.log1p(resident_total), jnp.log1p(density))


PAIR = 2
LANES = 128
SUBLANES = 8
INGEST_CHUNK = 256
RESIDENT_CHUNK = 256
HALVES = 2
MESH = pl.DeviceIdType.MESH
DENSE_VMEM = 55200 * 1024
SCORE_VMEM = 1024 * 1024


def dense_kernel(
    cycle, ids_ref, ingest_ref, resident_ref, resident_out, ingest_out,
    raw_ingest, raw_resident, load_sem, rows, bank, ids, by_resident, by_ingest, resident_sums, ingest_sums, resident_terms, ingest_terms,
    up_send, down_send, rows_recv, up_ids_send, down_ids_send, ids_recv, peer_send, peer_recv, core_send, core_recv,
    relay_send, relay_recv, part_send, part_recv, term_send, term_recv,
):
    line_size = cycle // PAIR
    me = lax.axis_index("blk")
    core = lax.axis_index("rep")
    line, side = me // PAIR, me % PAIR
    chunks = ingest_ref.shape[0] // INGEST_CHUNK
    held = resident_ref.shape[0]
    pieces = held // RESIDENT_CHUNK
    tile_rows = 2 * held
    steps = (line_size - 1) * chunks
    half_rows = INGEST_CHUNK // HALVES
    at_end = (line == 0) | (line == line_size - 1)
    below_end, above_end = line == 1, line == line_size - 2
    holds_back = line_size > 2

    def device(at_line, at_side, at_core):
        return {"blk": at_line * PAIR + at_side, "rep": at_core}

    sibling = device(line, side, 1 - core)
    peer = device(line, 1 - side, core)
    across = device(line, 1 - side, 1 - core)

    def remote(source, target, send, recv, where):
        return pltpu.make_async_remote_copy(
            src_ref=source, dst_ref=target, send_sem=send, recv_sem=recv, device_id=where, device_id_type=MESH
        )

    def row_copy(c, h, send, where):
        part = rows.at[c, pl.ds(h * half_rows, half_rows)]
        return remote(part, part, send.at[c, h], rows_recv.at[c, h], where)

    def id_copy(c, send, where):
        return remote(ids.at[c], ids.at[c], send.at[c], ids_recv.at[c], where)

    above, below = device(line + 1, side, core), device(line - 1, side, core)

    def up_copies(c):
        return [id_copy(c, up_ids_send, above)] + [row_copy(c, h, up_send, above) for h in range(HALVES)]

    def down_copies(c):
        return [id_copy(c, down_ids_send, below)] + [row_copy(c, h, down_send, below) for h in range(HALVES)]

    def start_all(copies):
        for copy in copies:
            copy.start()

    def peer_copy(m):
        return remote(
            bank.at[pl.ds(m * RESIDENT_CHUNK, RESIDENT_CHUNK)],
            bank.at[pl.ds(2 * held + m * RESIDENT_CHUNK, RESIDENT_CHUNK)],
            peer_send.at[m], peer_recv.at[m], peer,
        )

    def relay_copy(m):
        return remote(
            bank.at[pl.ds(2 * held + m * RESIDENT_CHUNK, RESIDENT_CHUNK)],
            bank.at[pl.ds(3 * held + m * RESIDENT_CHUNK, RESIDENT_CHUNK)],
            relay_send.at[m], relay_recv.at[m], sibling,
        )

    core_copy = remote(bank.at[pl.ds(0, held)], bank.at[pl.ds(held, held)], core_send, core_recv, sibling)

    def term_copy(other):
        return remote(
            ingest_sums.at[pl.ds(other * chunks, chunks)], ingest_terms.at[pl.ds(line * chunks, chunks)],
            term_send.at[other], term_recv.at[line], device(other, side, core),
        )

    def term_arrival(other):
        return remote(
            ingest_sums.at[pl.ds(other * chunks, chunks)], ingest_terms.at[pl.ds(other * chunks, chunks)],
            term_send.at[other], term_recv.at[other], device(other, side, core),
        )

    def part_copy(slot):
        return remote(
            resident_sums.at[slot], resident_terms.at[slot], part_send.at[slot], part_recv.at[slot],
            (None, sibling, peer, across)[slot],
        )

    barrier = pltpu.get_barrier_semaphore()
    for where in (sibling, peer, across):
        pl.semaphore_signal(barrier, inc=1, device_id=where, device_id_type=MESH)

    @pl.when(line > 0)
    def _():
        pl.semaphore_signal(barrier, inc=1, device_id=below, device_id_type=MESH)

    @pl.when(line + 1 < line_size)
    def _():
        pl.semaphore_signal(barrier, inc=1, device_id=above, device_id_type=MESH)

    ingest_load = pltpu.make_async_copy(ingest_ref, raw_ingest, load_sem.at[0])
    resident_load = pltpu.make_async_copy(resident_ref, raw_resident, load_sem.at[1])
    ids_load = pltpu.make_async_copy(ids_ref, ids.at[pl.ds(line * chunks, chunks)], load_sem.at[2])
    for load in (ingest_load, ids_load, resident_load):
        load.start()

    def unit(block):
        values = block.astype(jnp.float32)
        squares = jnp.sum(values * values, axis=-1, keepdims=True) + epsilon
        return (values * lax.rsqrt(squares)).astype(jnp.bfloat16)

    ingest_load.wait()
    for j in range(chunks):
        rows[line * chunks + j] = unit(raw_ingest[j * INGEST_CHUNK:(j + 1) * INGEST_CHUNK, :])
    ids_load.wait()
    pl.semaphore_wait(barrier, 3 + (line > 0).astype(jnp.int32) + (line + 1 < line_size).astype(jnp.int32))
    for j in range(chunks):
        kept = holds_back and j == chunks - 1

        @pl.when((line + 1 < line_size) & jnp.logical_not(above_end & kept))
        def _():
            start_all(up_copies(line * chunks + j))

        @pl.when((line > 0) & jnp.logical_not(below_end & kept))
        def _():
            start_all(down_copies(line * chunks + j))

    resident_load.wait()

    @pl.loop(0, pieces)
    def _(m):
        part = pl.ds(m * RESIDENT_CHUNK, RESIDENT_CHUNK)
        bank[part, :] = unit(raw_resident[part, :])

    for m in range(pieces):
        peer_copy(m).start()
    core_copy.start()
    by_resident[...] = jnp.zeros_like(by_resident)
    by_ingest[...] = jnp.zeros_like(by_ingest)

    scale = math.log2(math.e) / temper
    span = CL_OWN * cycle

    def work(c, first, last):
        @pl.loop(first, last)
        def _(tile):
            part = pl.ds(pl.multiple_of(tile * tile_rows, tile_rows), tile_rows)
            position = line * PAIR + jnp.where(tile == 0, side, 1 - side)
            gap = (position + 1) * CL_OWN - 1 - ids[c]
            gap = jnp.where(gap < 0, gap + span, gap)
            bias = jnp.where(gap < CL_OWN * (CYCLE_STEPS + 1), -scale, -1e30)
            scores = lax.dot_general(
                bank[part, :], rows[c], (((1,), (1,)), ((), ())), preferred_element_type=jnp.float32
            )
            kernel = jnp.exp2(scores * scale + bias)
            by_ingest[c] += jnp.sum(kernel.reshape(tile_rows // SUBLANES, SUBLANES, INGEST_CHUNK), axis=0)
            folded = kernel[:, :LANES]
            for n in range(1, INGEST_CHUNK // LANES):
                folded = folded + kernel[:, n * LANES:(n + 1) * LANES]
            by_resident[part, :] += folded

    core_copy.wait_recv()

    @pl.loop(0, chunks)
    def _(j):
        work(line * chunks + j, 0, 1)

    def gather_slot(slot):
        block = by_resident[slot * held:(slot + 1) * held, :]
        resident_sums[slot] = jnp.sum(block.T, axis=0, keepdims=True)

    def place(step):
        if not holds_back:
            return step
        turned = jnp.where(step == 0, 0, step + chunks - 1)
        late = step >= steps - chunks + 1
        return jnp.where(at_end & (chunks > 1), jnp.where(late, step - (steps - chunks), turned), step)

    def rank(spot):
        if not holds_back:
            return spot
        turned = jnp.where(spot == 0, 0, spot - chunks + 1)
        late = (spot >= 1) & (spot < chunks)
        return jnp.where(at_end & (chunks > 1), jnp.where(late, spot + steps - chunks, turned), spot)

    def take(step, tail=False):
        spot = place(step)
        hop, j = spot // chunks + 1, spot % chunks

        @pl.when(line - hop >= 0)
        def _():
            for copy in up_copies((line - hop) * chunks + j):
                copy.wait_recv()

                @pl.when(line + 1 < line_size)
                def _():
                    copy.start()

        @pl.when(line + hop < line_size)
        def _():
            for copy in down_copies((line + hop) * chunks + j):
                copy.wait_recv()

                @pl.when(line > 0)
                def _():
                    copy.start()

        if holds_back:
            @pl.when((step == (line_size - 2) * chunks - 1) & above_end)
            def _():
                start_all(up_copies(line * chunks + chunks - 1))

            @pl.when((step == (line_size - 2) * chunks - 1) & below_end)
            def _():
                start_all(down_copies(line * chunks + chunks - 1))

        def near_work(first, last):
            @pl.loop(0, 2)
            def _(way):
                other = line + (2 * way - 1) * hop

                @pl.when((other >= 0) & (other < line_size))
                def _():
                    work(other * chunks + j, first, last)

        if tail:
            near_work(1, 2)
            for slot in (3, 2):
                gather_slot(slot)
                part_copy(slot).start()
            near_work(0, 1)
            return

        @pl.when(step < pieces)
        def _():
            peer_copy(step).wait_recv()
            relay_copy(step).start()

        @pl.loop(0, 2)
        def _(way):
            other = line + (2 * way - 1) * hop

            @pl.when((other >= 0) & (other < line_size))
            def _():
                work(other * chunks + j, 0, jnp.where(step < pieces, 1, 2))

        @pl.when(step == pieces - 1)
        def _():
            for m in range(pieces):
                relay_copy(m).wait_recv()

            @pl.loop(0, line_size * chunks)
            def _(c):
                away = jnp.abs(c // chunks - line)
                arrived = rank((away - 1) * chunks + c % chunks)

                @pl.when((away == 0) | (arrived < pieces))
                def _():
                    work(c, 1, 2)

    @pl.loop(0, steps - 1)
    def _(step):
        take(step)

    def return_terms(near):
        for hop in range(1, line_size):
            other = (line + hop) % line_size
            away = jnp.abs(other - line)

            @pl.when((away == 1) if near else (away > 1))
            def _():
                theirs = pl.ds(other * chunks, chunks)
                ingest_sums[theirs] = jnp.sum(by_ingest[theirs], axis=1, keepdims=True)
                term_copy(other).start()

    early = pieces < steps
    if early:
        return_terms(False)
        take(steps - 1, tail=True)
    else:
        take(steps - 1)
        return_terms(False)
    return_terms(True)
    mine = pl.ds(line * chunks, chunks)
    ingest_sums[mine] = jnp.sum(by_ingest[mine], axis=1, keepdims=True)

    if not early:
        for slot in (3, 2):
            gather_slot(slot)
            part_copy(slot).start()
    gather_slot(1)
    part_copy(1).start()
    gather_slot(0)

    for c in range(line_size * chunks):
        @pl.when((c // chunks <= line) & (line + 1 < line_size))
        def _():
            for copy in up_copies(c):
                copy.wait_send()

        @pl.when((c // chunks >= line) & (line > 0))
        def _():
            for copy in down_copies(c):
                copy.wait_send()
    for m in range(pieces):
        peer_copy(m).wait_send()
        relay_copy(m).wait_send()
    core_copy.wait_send()

    resident_total = resident_sums[0]
    for slot in (1, 2, 3):
        part_copy(slot).wait()
        resident_total = resident_total + resident_terms[slot]
    resident_out[...] = resident_total
    ingest_total = ingest_sums[mine]
    for hop in range(1, line_size):
        other = (line + hop) % line_size
        term_arrival(other).wait_recv()
        ingest_total = ingest_total + ingest_terms[pl.ds(other * chunks, chunks)]
    ingest_out[...] = ingest_total
    for hop in range(1, line_size):
        other = (line + hop) % line_size
        term_copy(other).wait_send()


def score_kernel(resident_total, ingest_total, resident_score, ingest_score):
    resident_score[...] = jnp.log1p(resident_total[...])
    ingest_score[...] = jnp.log1p(ingest_total[...])


def dense_on_device(cycle, resident, ingest, cluster_ids):
    held, columns = resident.shape
    count = ingest.shape[0]
    chunks = count // INGEST_CHUNK
    blocks = cycle // PAIR * chunks
    line_size = cycle // PAIR
    pieces = held // RESIDENT_CHUNK
    dma = pltpu.SemaphoreType.DMA
    vmem = pl.BlockSpec(memory_space=pltpu.VMEM)
    resident_total, ingest_total = pl.pallas_call(
        functools.partial(dense_kernel, cycle),
        out_shape=(
            jax.ShapeDtypeStruct((1, held), jnp.float32),
            jax.ShapeDtypeStruct((chunks, 1, INGEST_CHUNK), jnp.float32),
        ),
        in_specs=[pl.BlockSpec(memory_space=pl.ANY)] * 3,
        out_specs=(vmem, vmem),
        scratch_shapes=[
            pltpu.VMEM((count, columns), jnp.bfloat16),
            pltpu.VMEM((held, columns), jnp.bfloat16),
            dma((3,)),
            pltpu.VMEM((blocks, INGEST_CHUNK, columns), jnp.bfloat16),
            pltpu.VMEM((4 * held, columns), jnp.bfloat16),
            pltpu.VMEM((blocks, 1, INGEST_CHUNK), jnp.int32),
            pltpu.VMEM((4 * held, LANES), jnp.float32),
            pltpu.VMEM((blocks, SUBLANES, INGEST_CHUNK), jnp.float32),
            pltpu.VMEM((4, 1, held), jnp.float32),
            pltpu.VMEM((blocks, 1, INGEST_CHUNK), jnp.float32),
            pltpu.VMEM((4, 1, held), jnp.float32),
            pltpu.VMEM((blocks, 1, INGEST_CHUNK), jnp.float32),
            dma((blocks, HALVES)), dma((blocks, HALVES)), dma((blocks, HALVES)),
            dma((blocks,)), dma((blocks,)), dma((blocks,)),
            dma((pieces,)), dma((pieces,)),
            dma, dma,
            dma((pieces,)), dma((pieces,)),
            dma((4,)), dma((4,)),
            dma((line_size,)), dma((line_size,)),
        ],
        compiler_params=pltpu.CompilerParams(
            collective_id=0, has_side_effects=True, vmem_limit_bytes=DENSE_VMEM
        ),
    )(cluster_ids.reshape(chunks, 1, INGEST_CHUNK), ingest, resident)
    resident_score, ingest_score = pl.pallas_call(
        score_kernel,
        out_shape=(
            jax.ShapeDtypeStruct(resident_total.shape, jnp.float32),
            jax.ShapeDtypeStruct(ingest_total.shape, jnp.float32),
        ),
        in_specs=[vmem] * 2,
        out_specs=(vmem, vmem),
        compiler_params=pltpu.CompilerParams(vmem_limit_bytes=SCORE_VMEM),
    )(resident_total, ingest_total)
    return (resident_score.reshape(held), ingest_score.reshape(count))


def solution(mesh):
    in_specs = (
        P(("groups", "blk", "rep"), None),
        P(("groups", "blk", "rep"), None),
        P(("groups", "blk", "rep")),
    )
    out_specs = (P(("groups", "blk", "rep")), P(("groups", "blk", "rep")))
    cycle = mesh.shape["blk"]
    dense = 2 * (CYCLE_STEPS + 1) >= cycle and cycle % PAIR == 0 and mesh.shape["rep"] == 2
    body = functools.partial(dense_on_device, cycle) if dense else on_device
    return jax.shard_map(
        body, mesh=mesh, in_specs=in_specs, out_specs=out_specs, check_vma=False
    )
```

```python
import functools
import math

import jax
import jax.numpy as jnp
from jax import lax
from jax.experimental import pallas as pl
from jax.experimental.pallas import tpu as pltpu
from jax.sharding import PartitionSpec as P

INGEST_DEV = 512
CL_OWN = 16
CYCLE_STEPS = 4


temper = 0.2
epsilon = 1e-06


def shifted(value, axis, steps):
    count = lax.axis_size(axis)
    pairs = [(source, (source + steps) % count) for source in range(count)]
    return lax.ppermute(value, axis, pairs)


def unit_rows(rows):
    values = rows.astype(jnp.float32)
    squares = jnp.sum(values * values, axis=-1, keepdims=True) + epsilon
    factor = lax.rsqrt(squares)
    return (values * factor).astype(jnp.bfloat16)


def kernel_sums(visitors, occupancy, residents):
    count_rows = visitors.shape[0]
    block_rows = 512
    num_blocks = count_rows // block_rows
    visit_blocks = visitors.reshape(num_blocks, block_rows, visitors.shape[1])
    live_blocks = occupancy.astype(jnp.float32).reshape(num_blocks, block_rows)

    def tile_sums(running, pieces):
        visit_tile, live_tile = pieces
        scores = jnp.einsum("vd,rd->vr", visit_tile, residents, preferred_element_type=jnp.float32)
        kernel = jnp.exp((scores - 1.0) / temper)
        return (running + jnp.sum(kernel * live_tile[:, None], axis=0), jnp.sum(kernel, axis=1))

    resident_part, visit_parts = lax.scan(
        tile_sums, jnp.zeros((residents.shape[0],), jnp.float32), (visit_blocks, live_blocks)
    )
    return (visit_parts.reshape(count_rows), resident_part)


def on_device(resident, ingest, cluster_ids):
    cycle_size = lax.axis_size("blk")
    slot_count = 3 * INGEST_DEV // (2 * cycle_size)
    columns = ingest.shape[1]
    owners = cluster_ids // CL_OWN
    onehot = (owners[:, None] == jnp.arange(cycle_size, dtype=jnp.int32)[None, :]).astype(jnp.int32)
    rank_within = jnp.sum((jnp.cumsum(onehot, axis=0) - onehot) * onehot, axis=1)
    targets = owners * slot_count + rank_within
    unit_ingest = unit_rows(ingest)
    outgoing = (
        jnp.zeros((cycle_size * slot_count, columns), jnp.bfloat16).at[targets].set(unit_ingest)
    )
    filled = (
        jnp.zeros((cycle_size * slot_count,), jnp.bfloat16)
        .at[targets]
        .set(jnp.ones((ingest.shape[0],), jnp.bfloat16))
    )
    arrived, present = (
        lax.all_to_all(
            outgoing.reshape(cycle_size, slot_count, columns),
            "blk",
            split_axis=0,
            concat_axis=0,
            tiled=True,
        ),
        lax.all_to_all(
            filled.reshape(cycle_size, slot_count), "blk", split_axis=0, concat_axis=0, tiled=True
        ),
    )
    visitors, marked = (
        lax.all_gather(
            arrived.reshape(cycle_size * slot_count, columns), "rep", axis=0, tiled=True
        ),
        lax.all_gather(present.reshape(cycle_size * slot_count), "rep", axis=0, tiled=True),
    )
    unit_resident = unit_rows(resident)
    visit_total = jnp.zeros((visitors.shape[0],), jnp.float32)
    resident_total = jnp.zeros((resident.shape[0],), jnp.float32)
    moving = unit_resident
    for rotation in range(CYCLE_STEPS + 1):
        if rotation > 0:
            moving = shifted(moving, "blk", -1)
            resident_total = shifted(resident_total, "blk", -1)
        visit_part, resident_part = kernel_sums(visitors, marked, moving)
        visit_total = visit_total + visit_part
        resident_total = resident_total + resident_part
    resident_total = shifted(resident_total, "blk", CYCLE_STEPS)
    own_sums = lax.psum_scatter(visit_total, "rep", scatter_dimension=0, tiled=True)
    returned = lax.all_to_all(
        own_sums.reshape(cycle_size, slot_count), "blk", split_axis=0, concat_axis=0, tiled=True
    )
    density = returned.reshape(cycle_size * slot_count)[targets]
    return (jnp.log1p(resident_total), jnp.log1p(density))


PAIR = 2
LANES = 128
SUBLANES = 8
INGEST_CHUNK = 256
RESIDENT_CHUNK = 256
HALVES = 2
MESH = pl.DeviceIdType.MESH
DENSE_VMEM = 55200 * 1024
SCORE_VMEM = 1024 * 1024


def dense_kernel(
    cycle, ids_ref, ingest_ref, resident_ref, resident_out, ingest_out,
    raw_ingest, raw_resident, load_sem, rows, bank, ids, by_resident, by_ingest, resident_sums, ingest_sums, resident_terms, ingest_terms,
    up_send, down_send, rows_recv, up_ids_send, down_ids_send, ids_recv, peer_send, peer_recv, core_send, core_recv,
    relay_send, relay_recv, part_send, part_recv, term_send, term_recv,
):
    line_size = cycle // PAIR
    me = lax.axis_index("blk")
    core = lax.axis_index("rep")
    line, side = me // PAIR, me % PAIR
    chunks = ingest_ref.shape[0] // INGEST_CHUNK
    held = resident_ref.shape[0]
    pieces = held // RESIDENT_CHUNK
    tile_rows = 2 * held
    steps = (line_size - 1) * chunks
    half_rows = INGEST_CHUNK // HALVES
    at_end = (line == 0) | (line == line_size - 1)
    below_end, above_end = line == 1, line == line_size - 2
    holds_back = line_size > 2

    def device(at_line, at_side, at_core):
        return {"blk": at_line * PAIR + at_side, "rep": at_core}

    sibling = device(line, side, 1 - core)
    peer = device(line, 1 - side, core)
    across = device(line, 1 - side, 1 - core)

    def remote(source, target, send, recv, where):
        return pltpu.make_async_remote_copy(
            src_ref=source, dst_ref=target, send_sem=send, recv_sem=recv, device_id=where, device_id_type=MESH
        )

    def row_copy(c, h, send, where):
        part = rows.at[c, pl.ds(h * half_rows, half_rows)]
        return remote(part, part, send.at[c, h], rows_recv.at[c, h], where)

    def id_copy(c, send, where):
        return remote(ids.at[c], ids.at[c], send.at[c], ids_recv.at[c], where)

    above, below = device(line + 1, side, core), device(line - 1, side, core)

    def up_copies(c):
        return [id_copy(c, up_ids_send, above)] + [row_copy(c, h, up_send, above) for h in range(HALVES)]

    def down_copies(c):
        return [id_copy(c, down_ids_send, below)] + [row_copy(c, h, down_send, below) for h in range(HALVES)]

    def start_all(copies):
        for copy in copies:
            copy.start()

    def peer_copy(m):
        return remote(
            bank.at[pl.ds(m * RESIDENT_CHUNK, RESIDENT_CHUNK)],
            bank.at[pl.ds(2 * held + m * RESIDENT_CHUNK, RESIDENT_CHUNK)],
            peer_send.at[m], peer_recv.at[m], peer,
        )

    def relay_copy(m):
        return remote(
            bank.at[pl.ds(2 * held + m * RESIDENT_CHUNK, RESIDENT_CHUNK)],
            bank.at[pl.ds(3 * held + m * RESIDENT_CHUNK, RESIDENT_CHUNK)],
            relay_send.at[m], relay_recv.at[m], sibling,
        )

    core_copy = remote(bank.at[pl.ds(0, held)], bank.at[pl.ds(held, held)], core_send, core_recv, sibling)

    def term_copy(other):
        return remote(
            ingest_sums.at[pl.ds(other * chunks, chunks)], ingest_terms.at[pl.ds(line * chunks, chunks)],
            term_send.at[other], term_recv.at[line], device(other, side, core),
        )

    def term_arrival(other):
        return remote(
            ingest_sums.at[pl.ds(other * chunks, chunks)], ingest_terms.at[pl.ds(other * chunks, chunks)],
            term_send.at[other], term_recv.at[other], device(other, side, core),
        )

    def part_copy(slot):
        return remote(
            resident_sums.at[slot], resident_terms.at[slot], part_send.at[slot], part_recv.at[slot],
            (None, sibling, peer, across)[slot],
        )

    barrier = pltpu.get_barrier_semaphore()
    for where in (sibling, peer):
        pl.semaphore_signal(barrier, inc=1, device_id=where, device_id_type=MESH)

    @pl.when(line > 0)
    def _():
        pl.semaphore_signal(barrier, inc=1, device_id=below, device_id_type=MESH)

    @pl.when(line + 1 < line_size)
    def _():
        pl.semaphore_signal(barrier, inc=1, device_id=above, device_id_type=MESH)

    ingest_load = pltpu.make_async_copy(ingest_ref, raw_ingest, load_sem.at[0])
    resident_load = pltpu.make_async_copy(resident_ref, raw_resident, load_sem.at[1])
    ids_load = pltpu.make_async_copy(ids_ref, ids.at[pl.ds(line * chunks, chunks)], load_sem.at[2])
    for load in (ingest_load, ids_load, resident_load):
        load.start()

    def unit(block):
        values = block.astype(jnp.float32)
        squares = jnp.sum(values * values, axis=-1, keepdims=True) + epsilon
        return (values * lax.rsqrt(squares)).astype(jnp.bfloat16)

    ingest_load.wait()
    for j in range(chunks):
        rows[line * chunks + j] = unit(raw_ingest[j * INGEST_CHUNK:(j + 1) * INGEST_CHUNK, :])
    ids_load.wait()
    pl.semaphore_wait(barrier, 2 + (line > 0).astype(jnp.int32) + (line + 1 < line_size).astype(jnp.int32))
    for j in range(chunks):
        kept = holds_back and j == chunks - 1

        @pl.when((line + 1 < line_size) & jnp.logical_not(above_end & kept))
        def _():
            start_all(up_copies(line * chunks + j))

        @pl.when((line > 0) & jnp.logical_not(below_end & kept))
        def _():
            start_all(down_copies(line * chunks + j))

    resident_load.wait()

    @pl.loop(0, pieces)
    def _(m):
        part = pl.ds(m * RESIDENT_CHUNK, RESIDENT_CHUNK)
        bank[part, :] = unit(raw_resident[part, :])

    for m in range(pieces):
        peer_copy(m).start()
    core_copy.start()
    by_resident[...] = jnp.zeros_like(by_resident)
    by_ingest[...] = jnp.zeros_like(by_ingest)

    scale = math.log2(math.e) / temper
    span = CL_OWN * cycle

    def work(c, first, last):
        @pl.loop(first, last)
        def _(tile):
            part = pl.ds(pl.multiple_of(tile * tile_rows, tile_rows), tile_rows)
            position = line * PAIR + jnp.where(tile == 0, side, 1 - side)
            gap = (position + 1) * CL_OWN - 1 - ids[c]
            gap = jnp.where(gap < 0, gap + span, gap)
            bias = jnp.where(gap < CL_OWN * (CYCLE_STEPS + 1), -scale, -1e30)
            scores = lax.dot_general(
                bank[part, :], rows[c], (((1,), (1,)), ((), ())), preferred_element_type=jnp.float32
            )
            kernel = jnp.exp2(scores * scale + bias)
            by_ingest[c] += jnp.sum(kernel.reshape(tile_rows // SUBLANES, SUBLANES, INGEST_CHUNK), axis=0)
            folded = kernel[:, :LANES]
            for n in range(1, INGEST_CHUNK // LANES):
                folded = folded + kernel[:, n * LANES:(n + 1) * LANES]
            by_resident[part, :] += folded

    core_copy.wait_recv()

    @pl.loop(0, chunks)
    def _(j):
        work(line * chunks + j, 0, 1)

    def gather_slot(slot):
        block = by_resident[slot * held:(slot + 1) * held, :]
        resident_sums[slot] = jnp.sum(block.T, axis=0, keepdims=True)

    def place(step):
        if not holds_back:
            return step
        turned = jnp.where(step == 0, 0, step + chunks - 1)
        late = step >= steps - chunks + 1
        return jnp.where(at_end & (chunks > 1), jnp.where(late, step - (steps - chunks), turned), step)

    def rank(spot):
        if not holds_back:
            return spot
        turned = jnp.where(spot == 0, 0, spot - chunks + 1)
        late = (spot >= 1) & (spot < chunks)
        return jnp.where(at_end & (chunks > 1), jnp.where(late, spot + steps - chunks, turned), spot)

    def take(step, tail=False):
        spot = place(step)
        hop, j = spot // chunks + 1, spot % chunks

        @pl.when(line - hop >= 0)
        def _():
            for copy in up_copies((line - hop) * chunks + j):
                copy.wait_recv()

                @pl.when(line + 1 < line_size)
                def _():
                    copy.start()

        @pl.when(line + hop < line_size)
        def _():
            for copy in down_copies((line + hop) * chunks + j):
                copy.wait_recv()

                @pl.when(line > 0)
                def _():
                    copy.start()

        if holds_back:
            @pl.when((step == (line_size - 2) * chunks - 1) & above_end)
            def _():
                start_all(up_copies(line * chunks + chunks - 1))

            @pl.when((step == (line_size - 2) * chunks - 1) & below_end)
            def _():
                start_all(down_copies(line * chunks + chunks - 1))

        def near_work(first, last):
            @pl.loop(0, 2)
            def _(way):
                other = line + (2 * way - 1) * hop

                @pl.when((other >= 0) & (other < line_size))
                def _():
                    work(other * chunks + j, first, last)

        if tail:
            near_work(1, 2)
            for slot in (3, 2):
                gather_slot(slot)
                part_copy(slot).start()
            near_work(0, 1)
            return

        @pl.when(step < pieces)
        def _():
            peer_copy(step).wait_recv()
            relay_copy(step).start()

        @pl.loop(0, 2)
        def _(way):
            other = line + (2 * way - 1) * hop

            @pl.when((other >= 0) & (other < line_size))
            def _():
                work(other * chunks + j, 0, jnp.where(step < pieces, 1, 2))

        @pl.when(step == pieces - 1)
        def _():
            for m in range(pieces):
                relay_copy(m).wait_recv()

            @pl.loop(0, line_size * chunks)
            def _(c):
                away = jnp.abs(c // chunks - line)
                arrived = rank((away - 1) * chunks + c % chunks)

                @pl.when((away == 0) | (arrived < pieces))
                def _():
                    work(c, 1, 2)

    @pl.loop(0, steps - 1)
    def _(step):
        take(step)

    def return_terms(near):
        for hop in range(1, line_size):
            other = (line + hop) % line_size
            away = jnp.abs(other - line)

            @pl.when((away == 1) if near else (away > 1))
            def _():
                theirs = pl.ds(other * chunks, chunks)
                ingest_sums[theirs] = jnp.sum(by_ingest[theirs], axis=1, keepdims=True)
                term_copy(other).start()

    early = pieces < steps
    if early:
        return_terms(False)
        take(steps - 1, tail=True)
    else:
        take(steps - 1)
        return_terms(False)
    return_terms(True)
    mine = pl.ds(line * chunks, chunks)
    ingest_sums[mine] = jnp.sum(by_ingest[mine], axis=1, keepdims=True)

    if not early:
        for slot in (3, 2):
            gather_slot(slot)
            part_copy(slot).start()
    gather_slot(1)
    part_copy(1).start()
    gather_slot(0)

    for c in range(line_size * chunks):
        @pl.when((c // chunks <= line) & (line + 1 < line_size))
        def _():
            for copy in up_copies(c):
                copy.wait_send()

        @pl.when((c // chunks >= line) & (line > 0))
        def _():
            for copy in down_copies(c):
                copy.wait_send()
    for m in range(pieces):
        peer_copy(m).wait_send()
        relay_copy(m).wait_send()
    core_copy.wait_send()

    resident_total = resident_sums[0]
    for slot in (1, 2, 3):
        part_copy(slot).wait()
        resident_total = resident_total + resident_terms[slot]
    resident_out[...] = resident_total
    ingest_total = ingest_sums[mine]
    for hop in range(1, line_size):
        other = (line + hop) % line_size
        term_arrival(other).wait_recv()
        ingest_total = ingest_total + ingest_terms[pl.ds(other * chunks, chunks)]
    ingest_out[...] = ingest_total
    for hop in range(1, line_size):
        other = (line + hop) % line_size
        term_copy(other).wait_send()


def score_kernel(resident_total, ingest_total, resident_score, ingest_score):
    resident_score[...] = jnp.log1p(resident_total[...])
    ingest_score[...] = jnp.log1p(ingest_total[...])


def dense_on_device(cycle, resident, ingest, cluster_ids):
    held, columns = resident.shape
    count = ingest.shape[0]
    chunks = count // INGEST_CHUNK
    blocks = cycle // PAIR * chunks
    line_size = cycle // PAIR
    pieces = held // RESIDENT_CHUNK
    dma = pltpu.SemaphoreType.DMA
    vmem = pl.BlockSpec(memory_space=pltpu.VMEM)
    resident_total, ingest_total = pl.pallas_call(
        functools.partial(dense_kernel, cycle),
        out_shape=(
            jax.ShapeDtypeStruct((1, held), jnp.float32),
            jax.ShapeDtypeStruct((chunks, 1, INGEST_CHUNK), jnp.float32),
        ),
        in_specs=[pl.BlockSpec(memory_space=pl.ANY)] * 3,
        out_specs=(vmem, vmem),
        scratch_shapes=[
            pltpu.VMEM((count, columns), jnp.bfloat16),
            pltpu.VMEM((held, columns), jnp.bfloat16),
            dma((3,)),
            pltpu.VMEM((blocks, INGEST_CHUNK, columns), jnp.bfloat16),
            pltpu.VMEM((4 * held, columns), jnp.bfloat16),
            pltpu.VMEM((blocks, 1, INGEST_CHUNK), jnp.int32),
            pltpu.VMEM((4 * held, LANES), jnp.float32),
            pltpu.VMEM((blocks, SUBLANES, INGEST_CHUNK), jnp.float32),
            pltpu.VMEM((4, 1, held), jnp.float32),
            pltpu.VMEM((blocks, 1, INGEST_CHUNK), jnp.float32),
            pltpu.VMEM((4, 1, held), jnp.float32),
            pltpu.VMEM((blocks, 1, INGEST_CHUNK), jnp.float32),
            dma((blocks, HALVES)), dma((blocks, HALVES)), dma((blocks, HALVES)),
            dma((blocks,)), dma((blocks,)), dma((blocks,)),
            dma((pieces,)), dma((pieces,)),
            dma, dma,
            dma((pieces,)), dma((pieces,)),
            dma((4,)), dma((4,)),
            dma((line_size,)), dma((line_size,)),
        ],
        compiler_params=pltpu.CompilerParams(
            collective_id=0, has_side_effects=True, vmem_limit_bytes=DENSE_VMEM
        ),
    )(cluster_ids.reshape(chunks, 1, INGEST_CHUNK), ingest, resident)
    resident_score, ingest_score = pl.pallas_call(
        score_kernel,
        out_shape=(
            jax.ShapeDtypeStruct(resident_total.shape, jnp.float32),
            jax.ShapeDtypeStruct(ingest_total.shape, jnp.float32),
        ),
        in_specs=[vmem] * 2,
        out_specs=(vmem, vmem),
        compiler_params=pltpu.CompilerParams(vmem_limit_bytes=SCORE_VMEM),
    )(resident_total, ingest_total)
    return (resident_score.reshape(held), ingest_score.reshape(count))


def solution(mesh):
    in_specs = (
        P(("groups", "blk", "rep"), None),
        P(("groups", "blk", "rep"), None),
        P(("groups", "blk", "rep")),
    )
    out_specs = (P(("groups", "blk", "rep")), P(("groups", "blk", "rep")))
    cycle = mesh.shape["blk"]
    dense = 2 * (CYCLE_STEPS + 1) >= cycle and cycle % PAIR == 0 and mesh.shape["rep"] == 2
    body = functools.partial(dense_on_device, cycle) if dense else on_device
    return jax.shard_map(
        body, mesh=mesh, in_specs=in_specs, out_specs=out_specs, check_vma=False
    )
```
